256 devices in a mesh: cell: 32 (over x, z), mem: 8 (over y, core).
Axes of the slice: x: 4, y: 4, z: 8, core: 2. Of those that a mesh axis runs over, the one named last changes fastest.
Arguments:
- logperm: float32 [128, 64, 64, 256], P('mem', 'cell'), may hold values from -4 to 4
- source: float32 [64, 64, 256], P('cell'), may hold values from -6 to 6
- obs_cells: int32 [4096], replicated, may hold values from 0 to 1048575
- obs_values: float32 [4096], replicated, may hold values from -2 to 2
- obs_prec: float32 [4096], replicated, may hold values from 0.1 to 10
Outputs:
- pressure: float32 [128, 64, 64, 256], P('mem', 'cell')
- analysis: float32 [128, 64, 64, 256], P('mem', 'cell')
The draws below stay inside these ranges and needn't reach their ends.
All inputs are finite; a program needn't handle non-finite values. Where the reference program divides by a largest or mean magnitude, that divisor is 1e-20 or more.
Results may differ from the reference program's by a relative error of at most 0.00015.
Values sent between devices are 32-bit elements; how exact they have to be, the bound alone decides.
No kernel may reach another device: no remote copies, remote signals or barrier semaphores. Data moves between devices by JAX's collectives and lax.ppermute only.
A program may use at most 128 MiB of HBM per device.

```python
import math
import jax
import jax.numpy as jnp
from jax import lax

M = 128
NOBS = 4096
ITERS = 4
NS_STEPS = 10
NY = 64
NZ = 256
NX = 64


def plant(drawn, stream_key, least, top_value):
    place = [jax.random.randint(jax.random.fold_in(stream_key, axis), (), 0, length) for axis, length in enumerate(drawn.shape)]
    main_axis = drawn.shape.index(max(drawn.shape))
    next_to = place[:main_axis] + [(place[main_axis] + 1) % drawn.shape[main_axis]] + place[main_axis + 1:]
    return drawn.at[tuple(place)].set(least).at[tuple(next_to)].set(top_value)


def shard_levels(rng, extent, cuts, least, largest):
    loudness = 1.0
    for axis_at, blocks in cuts:
        steps = jax.random.uniform(jax.random.fold_in(jax.random.fold_in(rng, 6), axis_at), (blocks,), jnp.float32, least / len(cuts), largest / len(cuts))
        loudness = loudness * jnp.repeat(jnp.exp(steps), extent[axis_at] // blocks).reshape((-1,) + (1,) * (len(extent) - 1 - axis_at))
    return loudness


def bell_draw(own_key, dims, spread, most, pieces=(), kind=jnp.bfloat16):
    entries = jax.random.normal(own_key, dims, jnp.float32) * spread
    if len(pieces) > 0:
        entries = shard_levels(own_key, dims, pieces, -0.22, 0.18) * entries
    return jnp.clip(entries, min=-most, max=most).astype(kind)


def setup_inputs(seed: int = 0) -> dict:
    key_list = jax.random.split(jax.random.key(seed), 6)
    return {
        "logperm": bell_draw(key_list[0], (M, NX, NY, NZ), 1.0, 4.0, ((0, 8), (1, 32)), jnp.float32),
        "source": bell_draw(key_list[1], (NX, NY, NZ), 1.0, 6.0, ((0, 32),), jnp.float32),
        "obs_cells": plant(jax.random.randint(key_list[2], (NOBS,), 0, NX * NY * NZ), jax.random.fold_in(key_list[2], 1), 0, (NX * NY * NZ) - 1).astype(jnp.int32),
        "obs_values": bell_draw(key_list[3], (NOBS,), 0.3, 2.0, (), jnp.float32),
        "obs_prec": jnp.clip(jnp.exp(jax.random.uniform(key_list[4], (NOBS,), jnp.float32, math.log(0.1), math.log(10.0))), 0.1, 10.0),
    }


CPRESS = 0.05
HIGH = lax.Precision.HIGHEST

def six_sides(padded):
    return (padded[:-2, 1:-1, 1:-1], padded[2:, 1:-1, 1:-1], padded[1:-1, :-2, 1:-1], padded[1:-1, 2:, 1:-1], padded[1:-1, 1:-1, :-2], padded[1:-1, 1:-1, 2:])

def member_pressure(member_field, source):
    mobility = jnp.exp(member_field)
    sides = six_sides(jnp.pad(mobility, 1))
    transmit = [jnp.sqrt(mobility * other) for other in sides]
    diagonal = CPRESS + transmit[0] + transmit[1] + transmit[2] + transmit[3] + transmit[4] + transmit[5]
    pressure = jnp.zeros_like(mobility)
    for sweep in range(ITERS):
        others = six_sides(jnp.pad(pressure, 1))
        inflow = transmit[0] * others[0] + transmit[1] * others[1] + transmit[2] * others[2]
        inflow = inflow + transmit[3] * others[3] + transmit[4] * others[4] + transmit[5] * others[5]
        pressure = (source + inflow) / diagonal
    return pressure

def build_transform(gram, innov):
    members = gram.shape[0]
    identity = jnp.eye(members, dtype=jnp.float32)
    scaled = identity + gram / (members - 1)
    bound = jnp.max(lax.optimization_barrier(jnp.sum(jnp.abs(scaled), axis=1)))
    root = scaled / bound
    inv_root = identity
    for sweep in range(NS_STEPS):
        factor = 1.5 * identity - 0.5 * jnp.dot(inv_root, root, precision=HIGH)
        root = jnp.dot(root, factor, precision=HIGH)
        inv_root = jnp.dot(factor, inv_root, precision=HIGH)
    inverse = jnp.dot(inv_root, inv_root, precision=HIGH) / bound
    shift_mean = jnp.dot(inverse, innov, precision=HIGH) / (members - 1)
    return inv_root / jnp.sqrt(bound) + shift_mean[:, None]

def reference(logperm, source, obs_cells, obs_values, obs_prec):
    pressure = lax.map(lambda member_field: member_pressure(member_field, source), logperm)
    predicted = jnp.take(pressure.reshape(M, -1), obs_cells, axis=1)
    mean_pred = lax.optimization_barrier(jnp.mean(predicted, axis=0))
    anomaly = predicted - mean_pred[None, :]
    gram = jnp.dot(anomaly * obs_prec[None, :], anomaly.T, precision=HIGH)
    innov = jnp.dot(anomaly, obs_prec * (obs_values - mean_pred), precision=HIGH)
    transform = build_transform(gram, innov)
    states = logperm.reshape(M, -1)
    mean_state = lax.optimization_barrier(jnp.mean(states, axis=0))
    analysis = mean_state[None, :] + jnp.dot(transform.T, states - mean_state[None, :], precision=HIGH)
    return (pressure, analysis.reshape(logperm.shape))
```

```python
import functools

import jax
import jax.numpy as jnp
from jax import lax
from jax.experimental import pallas as pl
from jax.experimental.pallas import tpu as pltpu
from jax.sharding import Mesh
from jax.sharding import PartitionSpec as P

M = 128
NOBS = 4096
NS_STEPS = 10
CPRESS = 0.05
HIGH = lax.Precision.HIGHEST
F32 = jnp.float32

NX, NZ, NMEM = 4, 8, 8
LAY = 2
MEM = M // NMEM
SUB = MEM // NZ
DEPTH = NZ * LAY
HALO = 4
FULL = DEPTH + 2 * HALO
NY, NW = 64, 256
CHUNK = 1280
BLOCK_BITS = 18

VM = pl.BlockSpec(memory_space=pltpu.VMEM)
SM = pl.BlockSpec(memory_space=pltpu.SMEM)
ANY = pl.BlockSpec(memory_space=pl.ANY)


def shape(*dims):
    return jax.ShapeDtypeStruct(dims, F32)


def call(kernel, outs, ins, specs, out_specs, scratch, flops, moved, name):
    return pl.pallas_call(
        kernel,
        out_shape=outs,
        in_specs=specs,
        out_specs=out_specs,
        scratch_shapes=scratch,
        cost_estimate=pl.CostEstimate(flops=flops, bytes_accessed=moved, transcendentals=0),
        compiler_params=pltpu.CompilerParams(vmem_limit_bytes=48 * 2**20),
        name=name,
    )(*ins)


def roots_kernel(where, *refs):
    parts, (h_ref, first_ref, last_ref) = refs[:NZ], refs[NZ:]
    z = where[0]
    for d in range(NZ):
        slab = lax.rem(z + d, NZ)
        for m in range(SUB):
            for a in range(LAY):
                h_ref[m, slab * LAY + a] = jnp.exp(0.5 * parts[d][m, a])
    first_ref[...] = h_ref[:, 0:HALO]
    last_ref[...] = h_ref[:, DEPTH - HALO : DEPTH]


def plane_sum(q):
    row = lax.broadcasted_iota(jnp.int32, q.shape, 0)
    lane = lax.broadcasted_iota(jnp.int32, q.shape, 1)
    total = jnp.where(row == 0, 0.0, pltpu.roll(q, 1, 0))
    total = total + jnp.where(row == NY - 1, 0.0, pltpu.roll(q, NY - 1, 0))
    total = total + jnp.where(lane == 0, 0.0, pltpu.roll(q, 1, 1))
    return total + jnp.where(lane == NW - 1, 0.0, pltpu.roll(q, NW - 1, 1))


def gather_block(where, cells, fields, rows, out, k):
    base = k * 128
    lanes = lax.broadcasted_iota(jnp.int32, (1, NW), 1)

    def one(o, carry):
        at = base + o
        cell = cells[at]
        owned = (at >= where[1]) & (at < where[2])
        layer = lax.shift_right_logical(cell, 14) & (DEPTH - 1)
        y = lax.shift_right_logical(cell, 8) & (NY - 1)
        lane = jnp.where(owned, cell & (NW - 1), -1)
        for m in range(SUB):
            row = fields[m, layer, pl.ds(y, 1), :]
            row = jnp.where(lanes == lane, row, 0.0)
            rows[m, pl.ds(o, 1), :] = row[:, :128] + row[:, 128:]
        return carry

    lax.fori_loop(0, 128, one, 0, unroll=8)
    for m in range(SUB):
        out[m, pl.ds(k, 1), :] = jnp.sum(rows[m].T, axis=0, keepdims=True)


def gather_all(where, cells, fields, rows, out):
    out[...] = jnp.zeros_like(out)
    low, high = where[1] // 128, (where[2] + 127) // 128

    @pl.loop(low, high)
    def _(k):
        gather_block(where, cells, fields, rows, out, k)


def sweeps_kernel(where, cells, h_ref, hl_ref, hr_ref, s_ref, sl_ref, sr_ref, *refs):
    outs, (pred_ref, h, rest, weight, qa, qb, press, rows) = refs[:NZ], refs[NZ:]
    for m in range(SUB):
        h[0:HALO] = hl_ref[m]
        h[HALO : HALO + DEPTH] = h_ref[m]
        h[HALO + DEPTH : FULL] = hr_ref[m]

        def prepare(j, source):
            root = h[j]
            near = h[j - 1] + h[j + 1] + plane_sum(root)
            inverse = 1.0 / (CPRESS + root * near)
            start = source * inverse
            rest[j] = start
            weight[j] = root * inverse
            qa[j] = root * start

        @pl.loop(1, HALO)
        def _(j):
            prepare(j, sl_ref[j])

        @pl.loop(0, DEPTH)
        def _(j):
            prepare(j + HALO, s_ref[j])

        @pl.loop(0, HALO - 1)
        def _(j):
            prepare(j + HALO + DEPTH, sr_ref[j])

        def pressure(j, q):
            return rest[j] + weight[j] * (q[j - 1] + q[j + 1] + plane_sum(q[j]))

        @pl.loop(2, FULL - 2)
        def _(j):
            qb[j] = h[j] * pressure(j, qa)

        @pl.loop(3, FULL - 3)
        def _(j):
            qa[j] = h[j] * pressure(j, qb)

        @pl.loop(0, DEPTH)
        def _(j):
            press[m, j] = pressure(j + HALO, qa)

    gather_all(where, cells, press, rows, pred_ref)
    z = where[0]
    for d in range(NZ):
        slab = lax.rem(z + d, NZ)
        for m in range(SUB):
            for a in range(LAY):
                outs[d][m, a] = press[m, slab * LAY + a]


def more_kernel(where, cells, *refs):
    parts, (pred_ref, press, rows) = refs[:NZ], refs[NZ:]
    z = where[0]
    for d in range(NZ):
        slab = lax.rem(z + d, NZ)
        for m in range(SUB):
            for a in range(LAY):
                press[m, slab * LAY + a] = parts[d][m, a]
    gather_all(where, cells, press, rows, pred_ref)


def gram_kernel(pred_ref, prec_ref, value_ref, out_ref):
    pred = pred_ref[...]
    prec = prec_ref[...]
    mean = jnp.sum(pred, axis=0, keepdims=True) * (1.0 / M)
    anomaly = pred - mean
    contract = (((1,), (1,)), ((), ()))
    out_ref[0:M] = lax.dot_general(
        anomaly * prec, anomaly, contract, precision=HIGH, preferred_element_type=F32
    )
    misfit = jnp.broadcast_to(prec * (value_ref[...] - mean), (8, CHUNK))
    out_ref[M : M + 8] = lax.dot_general(
        misfit, anomaly, contract, precision=HIGH, preferred_element_type=F32
    )


def dot(a, b):
    return jnp.dot(a, b, precision=HIGH, preferred_element_type=F32)


PIECES = 8
ROWS = 2 * NY // PIECES


def analysis_kernel(where, g0, g1, g2, g3, states, out, buffer, turned, sems):
    def piece(k):
        layer, first = divmod(k * ROWS, NY)
        return pltpu.make_async_copy(
            states.at[:, layer, pl.ds(first, ROWS), :],
            buffer.at[k],
            sems.at[k],
        )

    for k in range(PIECES):
        piece(k).start()

    sums = (g0[...] + g1[...]) + (g2[...] + g3[...])
    row = lax.broadcasted_iota(jnp.int32, (M, M), 0)
    column = lax.broadcasted_iota(jnp.int32, (M, M), 1)
    identity = jnp.where(row == column, 1.0, 0.0).astype(F32)
    scaled = identity + sums[0:M] / (M - 1)
    bound = jnp.max(jnp.sum(jnp.abs(scaled), axis=1, keepdims=True), axis=0, keepdims=True)
    root = scaled / bound
    inv_root = 1.5 * identity - 0.5 * root
    root = dot(root, inv_root)
    for step in range(1, NS_STEPS):
        factor = 1.5 * identity - 0.5 * dot(inv_root, root)
        if step < NS_STEPS - 1:
            root = dot(root, factor)
        inv_root = dot(factor, inv_root)
    contract = (((1,), (1,)), ((), ()))
    shift = sums[M : M + 8]
    for _ in range(2):
        shift = lax.dot_general(shift, inv_root, contract, precision=HIGH, preferred_element_type=F32)
    shift = shift[0:1] / bound / (M - 1)
    turned[...] = inv_root.T / jnp.sqrt(bound) + shift
    mine = turned[pl.ds(pl.multiple_of(where[3] * MEM, MEM), MEM), :]
    mine = mine + (1.0 - jnp.sum(mine, axis=1, keepdims=True)) * (1.0 / M)
    high = mine.astype(jnp.bfloat16)
    low = (mine - high.astype(F32)).astype(jnp.bfloat16)
    left = jnp.concatenate(
        [
            jnp.concatenate([high, high], axis=1),
            jnp.concatenate([low, jnp.zeros_like(low)], axis=1),
        ],
        axis=0,
    )
    for k in range(PIECES):
        piece(k).wait()
        layer, first = divmod(k * ROWS, NY)

        @pl.loop(0, ROWS)
        def _(r):
            state = buffer[k, :, r, :]
            upper = state.astype(jnp.bfloat16)
            lower = (state - upper.astype(F32)).astype(jnp.bfloat16)
            both = jnp.dot(
                left, jnp.concatenate([upper, lower], axis=0), preferred_element_type=F32
            )
            out[:, layer, first + r, :] = both[:MEM] + both[MEM:]


def shift_from(array, axis, size, by):
    return lax.ppermute(array, axis, [((i + by) % size, i) for i in range(size)])


def to_everyone(array, axis, size):
    copies = jnp.broadcast_to(array[None], (size, *array.shape))
    return lax.all_to_all(copies, axis, 0, 0, tiled=True)


def place_kernel(where, *refs):
    parts, (_, out, sems) = refs[:NZ], refs[NZ:]
    copies = []
    for d in range(NZ):
        group = lax.rem(where[0] + d, NZ)
        copies.append(
            pltpu.make_async_copy(parts[d], out.at[pl.ds(group * SUB, SUB)], sems.at[d])
        )
    for copy in copies:
        copy.start()
    for copy in copies:
        copy.wait()


def body(logperm, source, obs_cells, obs_values, obs_prec):
    x, z, mem = lax.axis_index("x"), lax.axis_index("z"), lax.axis_index(("y", "core"))
    states = lax.all_gather(logperm, ("y", "core"), axis=0, tiled=True)
    sources = lax.all_gather(source, "z", axis=0, tiled=True)

    def members_of(group):
        start = ((group & (NZ - 1)) * SUB, 0, 0, 0)
        sizes = (SUB, LAY, NY, NW)
        return lax.dynamic_slice(logperm, start, sizes, allow_negative_indices=False)

    parts = [None] * NZ
    for d in (4, 1, 7, 2, 6, 3, 5):
        parts[d] = shift_from(members_of(z - d), "z", NZ, d)
    parts[0] = members_of(z)

    cells, prec, values = lax.sort((obs_cells, obs_prec, obs_values), num_keys=1)
    block = lax.shift_right_logical(cells, BLOCK_BITS)
    counts = jnp.sum(block[None, :] == jnp.arange(NX)[:, None], axis=1).astype(jnp.int32)
    begin = jnp.sum(jnp.where(jnp.arange(NX) < x, counts, 0))
    count = jnp.sum(jnp.where(jnp.arange(NX) == x, counts, 0))
    most = jnp.max(counts)

    def window(done):
        want = jnp.minimum(begin + done, begin + count)
        first = jnp.minimum(want, NOBS - CHUNK)
        stop = jnp.minimum(want + CHUNK, begin + count)
        where = jnp.stack([z, want - first, jnp.maximum(stop - first, 0), mem]).astype(jnp.int32)
        cut = [lax.dynamic_slice(a, (first,), (CHUNK,), allow_negative_indices=False) for a in (cells, prec, values)]
        return where, cut[0], cut[1][None], cut[2][None]

    where, cells_0, prec_0, values_0 = window(0)
    big = SUB * DEPTH * NY * NW
    edge = shape(SUB, HALO, NY, NW)
    h, first, last = call(
        roots_kernel,
        [shape(SUB, DEPTH, NY, NW), edge, edge],
        [where, *parts],
        [SM] + [VM] * NZ,
        [VM] * 3,
        [],
        4 * big,
        12 * big,
        "roots",
    )
    up = [(i, i + 1) for i in range(NX - 1)]
    down = [(i + 1, i) for i in range(NX - 1)]
    h_left, h_right = lax.ppermute(last, "x", up), lax.ppermute(first, "x", down)
    s_left = lax.ppermute(sources[DEPTH - HALO :], "x", up)
    s_right = lax.ppermute(sources[:HALO], "x", down)

    part = shape(SUB, LAY, NY, NW)
    field = pltpu.VMEM((FULL, NY, NW), F32)
    pressed = pltpu.VMEM((SUB, DEPTH, NY, NW), F32)
    rows = pltpu.VMEM((SUB, 128, 128), F32)
    pred_shape = shape(SUB, CHUNK // 128, 128)
    *sent, pred = call(
        sweeps_kernel,
        [part] * NZ + [pred_shape],
        [where, cells_0, h, h_left, h_right, sources, s_left, s_right],
        [SM] * 2 + [VM] * 6,
        [VM] * (NZ + 1),
        [field] * 5 + [pressed, rows],
        64 * big,
        16 * big,
        "sweeps",
    )

    def gram_of(pred, prec_cut, value_cut):
        group = to_everyone(pred.reshape(SUB, CHUNK), "z", NZ).reshape(MEM, CHUNK)
        everyone = to_everyone(group, ("y", "core"), NMEM).reshape(M, CHUNK)
        return call(
            gram_kernel,
            shape(M + 8, M),
            [everyone, prec_cut, value_cut],
            [VM] * 3,
            VM,
            [],
            2 * M * M * CHUNK,
            4 * M * CHUNK,
            "gram",
        )

    def more(carry):
        done, total = carry
        where_n, cells_n, prec_n, values_n = window(done)
        pred_n = call(
            more_kernel,
            pred_shape,
            [where_n, cells_n, *sent],
            [SM] * 2 + [VM] * NZ,
            VM,
            [pressed, rows],
            big,
            8 * big,
            "more",
        )
        return done + CHUNK, total + gram_of(pred_n, prec_n, values_n)

    total = gram_of(pred, prec_0, values_0)
    _, total = lax.while_loop(lambda c: c[0] < most, more, (jnp.int32(CHUNK), total))
    others = [shift_from(total, "x", NX, d) for d in range(1, NX)]

    analysis = call(
        analysis_kernel,
        shape(MEM, LAY, NY, NW),
        [where, total, *others, states],
        [SM] + [VM] * NX + [ANY],
        VM,
        [
            pltpu.VMEM((PIECES, M, ROWS, NW), F32),
            pltpu.VMEM((M, M), F32),
            pltpu.SemaphoreType.DMA((PIECES,)),
        ],
        2 * M * MEM * LAY * NY * NW,
        4 * M * LAY * NY * NW,
        "analysis",
    )
    back = [sent[0]] + [shift_from(sent[NZ - d], "z", NZ, d) for d in range(1, NZ)]
    pressure = call(
        place_kernel,
        shape(MEM, LAY, NY, NW),
        [where, *back, analysis],
        [SM] + [VM] * NZ + [ANY],
        ANY,
        [pltpu.SemaphoreType.DMA((NZ,))],
        big,
        8 * big,
        "place",
    )
    return pressure, analysis


def solution(mesh):
    fine = Mesh(mesh.devices.reshape(NX, NZ, NMEM // 2, 2), ("x", "z", "y", "core"))
    cell, mem = ("x", "z"), ("y", "core")
    return jax.shard_map(
        body,
        mesh=fine,
        in_specs=(P(mem, cell, None, None), P(cell, None, None), P(), P(), P()),
        out_specs=(P(mem, cell, None, None), P(mem, cell, None, None)),
        check_vma=False,
    )
```

```python
import jax
import jax.numpy as jnp
from jax import lax
from jax.experimental import pallas as pl
from jax.experimental.pallas import tpu as pltpu
from jax.sharding import Mesh
from jax.sharding import PartitionSpec as P

M = 128
NOBS = 4096
NS_STEPS = 10
CPRESS = 0.05
HIGH = lax.Precision.HIGHEST
F32 = jnp.float32

NX, NZ, NMEM = 4, 8, 8
LAY = 2
MEM = M // NMEM
SUB = MEM // NZ
DEPTH = NZ * LAY
HALO = 4
FULL = DEPTH + 2 * HALO
GROUP = 4
ROOM = FULL + 6
NY, NW = 64, 256
HALVES = NW // 128
ROWS_OF = NY // NMEM
CHUNK = 1280
BLOCK_BITS = 18

VM = pl.BlockSpec(memory_space=pltpu.VMEM)
SM = pl.BlockSpec(memory_space=pltpu.SMEM)
ANY = pl.BlockSpec(memory_space=pl.ANY)
HBM = pl.BlockSpec(memory_space=pltpu.HBM)


def shape(*dims):
    return jax.ShapeDtypeStruct(dims, F32)


def call(kernel, outs, ins, specs, out_specs, scratch, flops, moved):
    return pl.pallas_call(
        kernel,
        out_shape=outs,
        in_specs=specs,
        out_specs=out_specs,
        scratch_shapes=scratch,
        cost_estimate=pl.CostEstimate(flops=flops, bytes_accessed=moved, transcendentals=0),
        compiler_params=pltpu.CompilerParams(vmem_limit_bytes=48 * 2**20),
    )(*ins)


def roots_kernel(where, *refs):
    parts, (h_ref, first_ref, last_ref, buffer, sems) = refs[:NZ], refs[NZ:]
    copies = [pltpu.make_async_copy(parts[d], buffer.at[d], sems.at[d]) for d in range(NZ)]
    for copy in copies:
        copy.start()
    for d in range(NZ):
        copies[d].wait()
        slab = (where[0] + d) & (NZ - 1)
        for m in range(SUB):
            for a in range(LAY):
                h_ref[m, slab * LAY + a] = jnp.exp(0.5 * buffer[d, m, a])
    first_ref[...] = h_ref[:, 0:HALO]
    last_ref[...] = h_ref[:, DEPTH - HALO : DEPTH]


TILES = [(i, half) for i in range(NY // 8) for half in range(NW // 128)]


def tile(i, half):
    return pl.ds(8 * i, 8), pl.ds(128 * half, 128)


def lane_sums(q, j, band, sums):
    value = q[pl.ds(j, GROUP)].reshape(GROUP * NY, NW)
    high = value.astype(jnp.bfloat16)
    low = (value - high.astype(F32)).astype(jnp.bfloat16)
    both = jnp.dot(jnp.concatenate([high, low], axis=0), band[...], preferred_element_type=F32)
    both = both[: GROUP * NY] + both[GROUP * NY :]
    sums[pl.ds(j, GROUP)] = both.reshape(GROUP, NY, NW)


def near_sums(q, sums, j):
    row = lax.broadcasted_iota(jnp.int32, (8, 128), 0)
    middle = {t: q[(j, *tile(*t))] for t in TILES}
    below = {t: pltpu.roll(middle[t], 1, 0) for t in TILES}
    above = {t: pltpu.roll(middle[t], 7, 0) for t in TILES}
    total = {}
    for i, half in TILES:
        t = (i, half)
        side = jnp.where(row == 0, below.get((i - 1, half), 0.0), below[t])
        side = side + jnp.where(row == 7, above.get((i + 1, half), 0.0), above[t])
        side = side + sums[(j, *tile(*t))]
        total[t] = side + (q[(j - 1, *tile(*t))] + q[(j + 1, *tile(*t))])
    return middle, total


def over_layers(q, band, sums, first, groups, step):
    lane_sums(q, first, band, sums)

    @pl.loop(0, groups)
    def _(c):
        j = first + c * GROUP
        for k in range(GROUP):
            step(j + k)
        lane_sums(q, j + GROUP, band, sums)


def gather_all(where, spots, lanes, press, found, out):
    out[...] = jnp.zeros_like(out)
    low, high = where[1] // 128, (where[2] + 127) // 128
    lane = lax.broadcasted_iota(jnp.int32, (1, 128), 1)
    flat = [press.at[m].reshape(HALVES * DEPTH * NY, 128) for m in range(SUB)]

    @pl.loop(low, high)
    def _(k):
        def one(o, carry):
            at = k * 128 + o
            spot, wanted = spots[at], lanes[at]
            for m in range(SUB):
                row = flat[m][pl.ds(spot, 1), :]
                found[m, pl.ds(o, 1), :] = jnp.where(lane == wanted, row, 0.0)
            return carry

        lax.fori_loop(0, 128, one, 0, unroll=16)
        for m in range(SUB):
            out[m, pl.ds(k, 1), :] = jnp.sum(found[m].T, axis=0, keepdims=True)


def sweeps_kernel(where, spots, lanes, h_ref, hl_ref, hr_ref, s_ref, *refs):
    outs, (pred_ref, h, qs, qw, qb, qc, rest, weight, sums, band, press, found) = refs[:NZ], refs[NZ:]
    row = lax.broadcasted_iota(jnp.int32, (NW, NW), 0)
    column = lax.broadcasted_iota(jnp.int32, (NW, NW), 1)
    band[...] = jnp.where(jnp.abs(row - column) == 1, 1.0, 0.0).astype(jnp.bfloat16)
    h[0] = jnp.zeros((NY, NW), F32)
    h[FULL + 1 : ROOM] = jnp.zeros((ROOM - FULL - 1, NY, NW), F32)

    @pl.loop(0, SUB)
    def _(m):
        h[1 : 1 + HALO] = hl_ref[m]
        h[1 + HALO : 1 + HALO + DEPTH] = h_ref[m]
        h[1 + HALO + DEPTH : 1 + FULL] = hr_ref[m]

        def prepare(j):
            root, near = near_sums(h, sums, j)
            for i, half in TILES:
                t, spot = (i, half), (j, *tile(i, half))
                inverse = 1.0 / (CPRESS + root[t] * near[t])
                start = s_ref[i, j - 1, :, pl.ds(128 * half, 128)] * inverse
                slope = root[t] * inverse
                rest[spot] = start
                weight[spot] = slope
                qs[spot] = root[t] * start
                qw[spot] = root[t] * slope

        def sweep_to(new, old):
            def step(j):
                _, near = near_sums(old, sums, j)
                for t in TILES:
                    spot = (j, *tile(*t))
                    new[spot] = qs[spot] + qw[spot] * near[t]

            return step

        def last(j):
            _, near = near_sums(qc, sums, j)
            for i, half in TILES:
                spot = (j, *tile(i, half))
                value = rest[spot] + weight[spot] * near[i, half]
                press[m, half, j - HALO - 1, pl.ds(8 * i, 8), :] = value

        over_layers(h, band, sums, 2, 6, prepare)
        over_layers(qs, band, sums, 3, 5, sweep_to(qb, qs))
        over_layers(qb, band, sums, 4, 5, sweep_to(qc, qb))
        over_layers(qc, band, sums, 5, 4, last)

    gather_all(where, spots, lanes, press, found, pred_ref)
    for d in range(NZ):
        slab = (where[0] + d) & (NZ - 1)
        for m in range(SUB):
            for a in range(LAY):
                for half in range(HALVES):
                    lanes_of = pl.ds(128 * half, 128)
                    outs[d][m, a, :, lanes_of] = press[m, half, slab * LAY + a]


def more_kernel(where, spots, lanes, *refs):
    parts, (pred_ref, press, found) = refs[:NZ], refs[NZ:]
    for d in range(NZ):
        slab = (where[0] + d) & (NZ - 1)
        for m in range(SUB):
            for a in range(LAY):
                for half in range(HALVES):
                    lanes_of = pl.ds(128 * half, 128)
                    press[m, half, slab * LAY + a] = parts[d][m, a, :, lanes_of]
    gather_all(where, spots, lanes, press, found, pred_ref)


def gram_kernel(pred_ref, prec_ref, value_ref, out_ref):
    pred = jnp.concatenate(
        [pred_ref[:, k].reshape(M, 128) for k in range(CHUNK // 128)], axis=1
    )
    prec = prec_ref[...]
    mean = jnp.sum(pred, axis=0, keepdims=True) * (1.0 / M)
    anomaly = pred - mean
    contract = (((1,), (1,)), ((), ()))
    out_ref[0:M] = lax.dot_general(
        anomaly * prec, anomaly, contract, precision=HIGH, preferred_element_type=F32
    )
    misfit = jnp.broadcast_to(prec * (value_ref[...] - mean), (8, CHUNK))
    out_ref[M : M + 8] = lax.dot_general(
        misfit, anomaly, contract, precision=HIGH, preferred_element_type=F32
    )


def dot(a, b):
    return jnp.dot(a, b, precision=HIGH, preferred_element_type=F32)


PIECES = 8
ROWS = LAY * NY // PIECES


BLOCKS = [(0, 0), (1, 0), (3, 0), (2, 0), (2, MEM // 2)]


def analysis_kernel(where, g0, g1, g2, g3, *refs):
    states, (out, buffer, done, turned, sems, out_sems) = refs[: 2 * len(BLOCKS)], refs[2 * len(BLOCKS) :]

    def place(k, half):
        layer, first = k // (NY // ROWS), pl.multiple_of(k % (NY // ROWS) * ROWS, ROWS)
        return (slice(None), layer, pl.ds(first, ROWS), pl.ds(half * 128, 128))

    def pieces(k, half):
        y, core = where[3] // 2, where[3] & 1
        copies = []
        for n, source in enumerate(states):
            step, first = BLOCKS[n % len(BLOCKS)]
            group = ((y + step) & 3) * 2 + (core if n < len(BLOCKS) else 1 - core)
            rows = pl.ds(group * MEM + first, source.shape[0])
            there = buffer.at[k, half, rows]
            copies.append(pltpu.make_async_copy(source.at[place(k, half)], there, sems.at[k, half, n]))
        return copies

    def result(k, half):
        return pltpu.make_async_copy(
            done.at[k, half], out.at[place(k, half)], out_sems.at[k, half]
        )

    @pl.loop(0, PIECES)
    def _(k):
        for half in range(HALVES):
            for copy in pieces(k, half):
                copy.start()

    sums = (g0[...] + g1[...]) + (g2[...] + g3[...])
    row = lax.broadcasted_iota(jnp.int32, (M, M), 0)
    column = lax.broadcasted_iota(jnp.int32, (M, M), 1)
    identity = jnp.where(row == column, 1.0, 0.0).astype(F32)
    scaled = identity + sums[0:M] / (M - 1)
    bound = jnp.max(jnp.sum(jnp.abs(scaled), axis=1, keepdims=True), axis=0, keepdims=True)
    root = scaled / bound
    inv_root = 1.5 * identity - 0.5 * root
    root = dot(root, inv_root)
    for step in range(1, NS_STEPS):
        factor = 1.5 * identity - 0.5 * dot(inv_root, root)
        if step < NS_STEPS - 1:
            root = dot(root, factor)
        inv_root = dot(factor, inv_root)
    contract = (((1,), (1,)), ((), ()))
    shift = sums[M : M + 8]
    for _ in range(2):
        shift = lax.dot_general(shift, inv_root, contract, precision=HIGH, preferred_element_type=F32)
    shift = shift[0:1] / bound / (M - 1)
    turned[...] = inv_root.T / jnp.sqrt(bound) + shift
    mine = turned[pl.ds(pl.multiple_of(where[3] * MEM, MEM), MEM), :]
    mine = mine + (1.0 - jnp.sum(mine, axis=1, keepdims=True)) * (1.0 / M)
    high = mine.astype(jnp.bfloat16)
    low = (mine - high.astype(F32)).astype(jnp.bfloat16)
    left = jnp.concatenate(
        [
            jnp.concatenate([high, high], axis=1),
            jnp.concatenate([low, jnp.zeros_like(low)], axis=1),
        ],
        axis=0,
    )

    @pl.loop(0, PIECES)
    def _(k):
        for half in range(HALVES):
            for copy in pieces(k, half):
                copy.wait()
        given = [buffer.at[k, half].reshape(M * ROWS, 128) for half in range(HALVES)]
        taken = [done.at[k, half].reshape(MEM * ROWS, 128) for half in range(HALVES)]
        for r in range(ROWS):
            state = jnp.concatenate([g[pl.ds(r, M, stride=ROWS), :] for g in given], axis=1)
            upper = state.astype(jnp.bfloat16)
            lower = (state - upper.astype(F32)).astype(jnp.bfloat16)
            both = jnp.dot(
                left, jnp.concatenate([upper, lower], axis=0), preferred_element_type=F32
            )
            both = both[:MEM] + both[MEM:]
            for half in range(HALVES):
                taken[half][pl.ds(r, MEM, stride=ROWS), :] = both[:, half * 128 : half * 128 + 128]
        for half in range(HALVES):
            result(k, half).start()

    for k in range(PIECES):
        for half in range(HALVES):
            result(k, half).wait()


BIG = SUB * DEPTH * NY * NW
PART = shape(SUB, LAY, NY, NW)
PRED = shape(SUB, CHUNK // 128, 128)
PRESSED = pltpu.VMEM((SUB, HALVES, DEPTH, NY, 128), F32)
FOUND = pltpu.VMEM((SUB, 128, 128), F32)


def sweep(*ins):
    return call(
        sweeps_kernel,
        [PART] * NZ + [PRED],
        ins,
        [SM] * 3 + [VM] * 4,
        [VM] * (NZ + 1),
        [pltpu.VMEM((ROOM, NY, NW), F32)] * 8
        + [pltpu.VMEM((NW, NW), jnp.bfloat16), PRESSED, FOUND],
        64 * BIG,
        16 * BIG,
    )


def analyse(where, sums, states):
    return call(
        analysis_kernel,
        shape(MEM, LAY, NY, NW),
        [where, *sums, *states],
        [SM] + [VM] * NX + [HBM] * (2 * len(BLOCKS)),
        ANY,
        [
            pltpu.VMEM((PIECES, HALVES, M, ROWS, 128), F32),
            pltpu.VMEM((PIECES, HALVES, MEM, ROWS, 128), F32),
            pltpu.VMEM((M, M), F32),
            pltpu.SemaphoreType.DMA((PIECES, HALVES, 2 * len(BLOCKS))),
            pltpu.SemaphoreType.DMA((PIECES, HALVES)),
        ],
        2 * M * MEM * LAY * NY * NW,
        4 * M * LAY * NY * NW,
    )


def shift_from(array, axis, size, by):
    return lax.ppermute(array, axis, [((i + by) % size, i) for i in range(size)])


def round_z(array):
    return [array] + [shift_from(array, "z", NZ, d) for d in range(1, NZ)]


def across_z(array):
    copies = lax.all_to_all(jnp.broadcast_to(array, (NZ, *array.shape)), "z", 0, 0, tiled=True)
    return [copies]


def strips_kernel(strips, out):
    for copy in range(NMEM):
        for slab in range(NZ):
            out[copy, LAY * slab : LAY * slab + LAY] = strips[slab]


def preds_kernel(where, *refs):
    parts, out = refs[:NZ], refs[NZ]
    for d in range(NZ):
        first = ((where[0] + d) & (NZ - 1)) * SUB
        for m in range(SUB):
            for k in range(CHUNK // 128):
                out[0, k, pl.ds(first + m, 1), :] = parts[d][m, pl.ds(k, 1), :]
    for copy in range(1, NMEM):
        out[copy] = out[0]


def to_mem(kernel, first, parts, dims):
    copies = call(
        kernel,
        shape(NMEM, *dims),
        [*first, *parts],
        [SM] * len(first) + [VM] * len(parts),
        VM,
        [],
        2**20,
        2**20,
    )
    return lax.all_to_all(copies, ("y", "core"), 0, 0, tiled=True)


def place_kernel(where, *refs):
    parts, (_, out, sems) = refs[:NZ], refs[NZ:]
    copies = []
    for d in range(NZ):
        group = (where[0] + d) & (NZ - 1)
        copies.append(
            pltpu.make_async_copy(parts[d], out.at[pl.ds(group * SUB, SUB)], sems.at[d])
        )
    for copy in copies:
        copy.start()
    for copy in copies:
        copy.wait()


def body(logperm, source, obs_cells, obs_values, obs_prec):
    x, z, mem = lax.axis_index("x"), lax.axis_index("z"), lax.axis_index(("y", "core"))

    def swapped(array):
        return lax.ppermute(array, "core", [(0, 1), (1, 0)])

    half = MEM // 2
    after, before = shift_from(logperm, "y", 4, 1), shift_from(logperm, "y", 4, 3)
    far_a, far_b = shift_from(after[:half], "y", 4, 1), shift_from(before[half:], "y", 4, 3)
    near = [logperm, after, before, far_a, far_b]
    states = near + [swapped(array) for array in near]

    def members_of(group):
        start = ((group & (NZ - 1)) * SUB, 0, 0, 0)
        sizes = (SUB, LAY, NY, NW)
        return lax.dynamic_slice(logperm, start, sizes, allow_negative_indices=False)

    parts = [None] * NZ
    for d in (4, 1, 7, 2, 6, 3, 5):
        parts[d] = shift_from(members_of(z - d), "z", NZ, d)
    parts[0] = members_of(z)

    strip = lax.dynamic_slice(
        source, (0, mem * ROWS_OF, 0), (LAY, ROWS_OF, NW), allow_negative_indices=False
    )
    strips = across_z(strip)
    sources = to_mem(strips_kernel, [], strips, (DEPTH, ROWS_OF, NW))
    at_z = [jnp.reshape(z, (1,)).astype(jnp.int32)]
    at_start = [jnp.zeros((1,), jnp.int32)]

    cells, prec, values = lax.sort((obs_cells, obs_prec, obs_values), num_keys=1)
    block = lax.shift_right_logical(cells, BLOCK_BITS)
    counts = jnp.sum(block[None, :] == jnp.arange(NX)[:, None], axis=1).astype(jnp.int32)
    begin = jnp.sum(jnp.where(jnp.arange(NX) < x, counts, 0))
    count = jnp.sum(jnp.where(jnp.arange(NX) == x, counts, 0))
    most = jnp.max(counts)

    def window(done):
        want = jnp.minimum(begin + done, begin + count)
        first = jnp.minimum(want, NOBS - CHUNK)
        stop = jnp.minimum(want + CHUNK, begin + count)
        where = jnp.stack([z, want - first, jnp.maximum(stop - first, 0), mem]).astype(jnp.int32)

        def cut(array):
            return lax.dynamic_slice(array, (first,), (CHUNK,), allow_negative_indices=False)

        at = cut(cells)
        half = lax.shift_right_logical(at, 7) & (HALVES - 1)
        spots = half * (DEPTH * NY) + (lax.shift_right_logical(at, 8) & (DEPTH * NY - 1))
        place = jnp.arange(CHUNK, dtype=jnp.int32)
        lanes = jnp.where((place >= where[1]) & (place < where[2]), at & 127, -1)
        return where, spots, lanes, cut(prec)[None], cut(values)[None]

    where, spots_0, lanes_0, prec_0, values_0 = window(0)
    edge = shape(SUB, HALO, NY, NW)
    h, first, last = call(
        roots_kernel,
        [shape(SUB, DEPTH, NY, NW), edge, edge],
        [where, *parts],
        [SM] + [HBM] * NZ,
        [VM] * 3,
        [pltpu.VMEM((NZ, SUB, LAY, NY, NW), F32), pltpu.SemaphoreType.DMA((NZ,))],
        4 * BIG,
        12 * BIG,
    )
    up = [(i, i + 1) for i in range(NX - 1)]
    down = [(i + 1, i) for i in range(NX - 1)]
    h_left, h_right = lax.ppermute(last, "x", up), lax.ppermute(first, "x", down)
    s_left = lax.ppermute(sources[:, DEPTH - HALO :], "x", up)
    s_right = lax.ppermute(sources[:, :HALO], "x", down)

    spare = jnp.zeros((NMEM, 2, ROWS_OF, NW), F32)
    sources = jnp.concatenate([s_left, sources, s_right, spare], axis=1)
    *sent, pred = sweep(where, spots_0, lanes_0, h, h_left, h_right, sources)

    def gram_of(first, parts, prec_cut, value_cut):
        everyone = to_mem(preds_kernel, first, parts, (CHUNK // 128, MEM, 128))
        return call(
            gram_kernel,
            shape(M + 8, M),
            [everyone, prec_cut, value_cut],
            [VM] * 3,
            VM,
            [],
            2 * M * M * CHUNK,
            4 * M * CHUNK,
        )

    def more(carry):
        done, total = carry
        where_n, spots_n, lanes_n, prec_n, values_n = window(done)
        pred_n = call(
            more_kernel,
            PRED,
            [where_n, spots_n, lanes_n, *sent],
            [SM] * 3 + [VM] * NZ,
            VM,
            [PRESSED, FOUND],
            BIG,
            8 * BIG,
        )
        gathered = across_z(pred_n)[0]
        split = [gathered[d] for d in range(NZ)]
        return done + CHUNK, total + gram_of(at_start, split, prec_n, values_n)

    total = gram_of(at_z, round_z(pred), prec_0, values_0)
    _, total = lax.while_loop(lambda c: c[0] < most, more, (jnp.int32(CHUNK), total))
    others = [shift_from(total, "x", NX, d) for d in range(1, NX)]

    analysis = analyse(where, [total, *others], states)
    back = [sent[0]] + [shift_from(sent[NZ - d], "z", NZ, d) for d in range(1, NZ)]
    pressure = call(
        place_kernel,
        shape(MEM, LAY, NY, NW),
        [where, *back, analysis],
        [SM] + [VM] * NZ + [ANY],
        ANY,
        [pltpu.SemaphoreType.DMA((NZ,))],
        BIG,
        8 * BIG,
    )
    return pressure, analysis


def solution(mesh):
    fine = Mesh(mesh.devices.reshape(NX, NZ, NMEM // 2, 2), ("x", "z", "y", "core"))
    cell, mem = ("x", "z"), ("y", "core")
    return jax.shard_map(
        body,
        mesh=fine,
        in_specs=(P(mem, cell, None, None), P(cell, None, None), P(), P(), P()),
        out_specs=(P(mem, cell, None, None), P(mem, cell, None, None)),
        check_vma=False,
    )
```

```python
import jax
import jax.numpy as jnp
from jax import lax
from jax.experimental import pallas as pl
from jax.experimental.pallas import tpu as pltpu
from jax.sharding import Mesh
from jax.sharding import PartitionSpec as P

M = 128
NOBS = 4096
NS_STEPS = 10
CPRESS = 0.05
HIGH = lax.Precision.HIGHEST
F32 = jnp.float32

NX, NZ, NMEM = 4, 8, 8
LAY = 2
MEM = M // NMEM
SUB = MEM // NZ
DEPTH = NZ * LAY
HALO = 4
FULL = DEPTH + 2 * HALO
GROUP = 4
ROOM = FULL + 6
NY, NW = 64, 256
HALVES = NW // 128
ROWS_OF = NY // NMEM
CHUNK = 1280
BLOCK_BITS = 18

VM = pl.BlockSpec(memory_space=pltpu.VMEM)
SM = pl.BlockSpec(memory_space=pltpu.SMEM)
ANY = pl.BlockSpec(memory_space=pl.ANY)
HBM = pl.BlockSpec(memory_space=pltpu.HBM)


def shape(*dims):
    return jax.ShapeDtypeStruct(dims, F32)


def call(kernel, outs, ins, specs, out_specs, scratch, flops, moved):
    return pl.pallas_call(
        kernel,
        out_shape=outs,
        in_specs=specs,
        out_specs=out_specs,
        scratch_shapes=scratch,
        cost_estimate=pl.CostEstimate(flops=flops, bytes_accessed=moved, transcendentals=0),
        compiler_params=pltpu.CompilerParams(vmem_limit_bytes=48 * 2**20),
    )(*ins)


def roots_kernel(where, *refs):
    parts, (h_ref, first_ref, last_ref, buffer, sems) = refs[:NZ], refs[NZ:]
    copies = [pltpu.make_async_copy(parts[d], buffer.at[d], sems.at[d]) for d in range(NZ)]
    for copy in copies:
        copy.start()
    for d in range(NZ):
        copies[d].wait()
        slab = (where[0] + d) & (NZ - 1)
        for m in range(SUB):
            for a in range(LAY):
                h_ref[m, slab * LAY + a] = jnp.exp(0.5 * buffer[d, m, a])
    first_ref[...] = h_ref[:, 0:HALO]
    last_ref[...] = h_ref[:, DEPTH - HALO : DEPTH]


TILES = [(i, half) for i in range(NY // 8) for half in range(NW // 128)]


def tile(i, half):
    return pl.ds(8 * i, 8), pl.ds(128 * half, 128)


def lane_sums(q, j, band, sums):
    value = q[pl.ds(j, GROUP)].reshape(GROUP * NY, NW)
    high = value.astype(jnp.bfloat16)
    low = (value - high.astype(F32)).astype(jnp.bfloat16)
    both = jnp.dot(jnp.concatenate([high, low], axis=0), band[...], preferred_element_type=F32)
    both = both[: GROUP * NY] + both[GROUP * NY :]
    sums[pl.ds(j, GROUP)] = both.reshape(GROUP, NY, NW)


def near_sums(q, sums, j):
    row = lax.broadcasted_iota(jnp.int32, (8, 128), 0)
    middle = {t: q[(j, *tile(*t))] for t in TILES}
    below = {t: pltpu.roll(middle[t], 1, 0) for t in TILES}
    above = {t: pltpu.roll(middle[t], 7, 0) for t in TILES}
    total = {}
    for i, half in TILES:
        t = (i, half)
        side = jnp.where(row == 0, below.get((i - 1, half), 0.0), below[t])
        side = side + jnp.where(row == 7, above.get((i + 1, half), 0.0), above[t])
        side = side + sums[(j, *tile(*t))]
        total[t] = side + (q[(j - 1, *tile(*t))] + q[(j + 1, *tile(*t))])
    return middle, total


def over_layers(q, band, sums, first, groups, step):
    lane_sums(q, first, band, sums)

    @pl.loop(0, groups)
    def _(c):
        j = first + c * GROUP
        for k in range(GROUP):
            step(j + k)
        lane_sums(q, j + GROUP, band, sums)


def gather_all(where, spots, lanes, press, found, copies):
    out = copies.at[0]
    out[...] = jnp.zeros_like(out)
    low, high = where[1] // 128, (where[2] + 127) // 128
    lane = lax.broadcasted_iota(jnp.int32, (1, 128), 1)
    flat = [press.at[m].reshape(HALVES * DEPTH * NY, 128) for m in range(SUB)]

    @pl.loop(low, high)
    def _(k):
        def one(o, carry):
            at = k * 128 + o
            spot, wanted = spots[at], lanes[at]
            for m in range(SUB):
                row = flat[m][pl.ds(spot, 1), :]
                found[m, pl.ds(o, 1), :] = jnp.where(lane == wanted, row, 0.0)
            return carry

        lax.fori_loop(0, 128, one, 0, unroll=16)
        for m in range(SUB):
            out[k, m : m + 1, :] = jnp.sum(found[m].T, axis=0, keepdims=True)

    for copy in range(1, NZ):
        copies[copy] = out[...]


def sweeps_kernel(where, spots, lanes, h_ref, hl_ref, hr_ref, s_ref, *refs):
    out, pred_ref, h, qs, qw, qb, qc, rest, weight, sums, band, press, found, sems = refs

    def results(m):
        copies = []
        for slab in range(NZ):
            for half in range(HALVES):
                done = press.at[m, half, pl.ds(slab * LAY, LAY)]
                place = out.at[slab, m, :, :, pl.ds(128 * half, 128)]
                copies.append(pltpu.make_async_copy(done, place, sems.at[m, half, slab]))
        return copies

    row = lax.broadcasted_iota(jnp.int32, (NW, NW), 0)
    column = lax.broadcasted_iota(jnp.int32, (NW, NW), 1)
    band[...] = jnp.where(jnp.abs(row - column) == 1, 1.0, 0.0).astype(jnp.bfloat16)
    h[0] = jnp.zeros((NY, NW), F32)
    h[FULL + 1 : ROOM] = jnp.zeros((ROOM - FULL - 1, NY, NW), F32)

    @pl.loop(0, SUB)
    def _(m):
        h[1 : 1 + HALO] = hl_ref[m]
        h[1 + HALO : 1 + HALO + DEPTH] = h_ref[m]
        h[1 + HALO + DEPTH : 1 + FULL] = hr_ref[m]

        def prepare(j):
            root, near = near_sums(h, sums, j)
            for i, half in TILES:
                t, spot = (i, half), (j, *tile(i, half))
                inverse = 1.0 / (CPRESS + root[t] * near[t])
                start = s_ref[i, j - 1, :, pl.ds(128 * half, 128)] * inverse
                slope = root[t] * inverse
                rest[spot] = start
                weight[spot] = slope
                qs[spot] = root[t] * start
                qw[spot] = root[t] * slope

        def sweep_to(new, old):
            def step(j):
                _, near = near_sums(old, sums, j)
                for t in TILES:
                    spot = (j, *tile(*t))
                    new[spot] = qs[spot] + qw[spot] * near[t]

            return step

        def last(j):
            _, near = near_sums(qc, sums, j)
            for i, half in TILES:
                spot = (j, *tile(i, half))
                value = rest[spot] + weight[spot] * near[i, half]
                press[m, half, j - HALO - 1, pl.ds(8 * i, 8), :] = value

        over_layers(h, band, sums, 2, 6, prepare)
        over_layers(qs, band, sums, 3, 5, sweep_to(qb, qs))
        over_layers(qb, band, sums, 4, 5, sweep_to(qc, qb))
        over_layers(qc, band, sums, 5, 4, last)

        for copy in results(m):
            copy.start()

    gather_all(where, spots, lanes, press, found, pred_ref)

    @pl.loop(0, SUB)
    def _(m):
        for copy in results(m):
            copy.wait()


def more_kernel(where, spots, lanes, parts, pred_ref, press, found):
    for slab in range(NZ):
        for m in range(SUB):
            for half in range(HALVES):
                lanes_of = pl.ds(128 * half, 128)
                press[m, half, slab * LAY : slab * LAY + LAY] = parts[slab, m, :, :, lanes_of]
    gather_all(where, spots, lanes, press, found, pred_ref)


def gram_kernel(mem, *refs):
    parts, (prec_ref, value_ref, out_ref, preds) = refs[:NMEM], refs[NMEM:]
    for e in range(NMEM):
        preds[group_at(mem[0], e)] = parts[e][...]
    pred = jnp.concatenate([preds[:, k].reshape(M, 128) for k in range(CHUNK // 128)], axis=1)
    prec = prec_ref[...]
    mean = jnp.sum(pred, axis=0, keepdims=True) * (1.0 / M)
    anomaly = pred - mean
    contract = (((1,), (1,)), ((), ()))
    out_ref[0:M] = lax.dot_general(
        anomaly * prec, anomaly, contract, precision=HIGH, preferred_element_type=F32
    )
    misfit = jnp.broadcast_to(prec * (value_ref[...] - mean), (8, CHUNK))
    out_ref[M : M + 8] = lax.dot_general(
        misfit, anomaly, contract, precision=HIGH, preferred_element_type=F32
    )


def dot(a, b):
    return jnp.dot(a, b, precision=HIGH, preferred_element_type=F32)


PIECES = 8
ROWS = LAY * NY // PIECES


BLOCKS = [(0, 0), (1, 0), (3, 0), (2, 0), (2, MEM // 2)]


def analysis_kernel(where, g0, g1, g2, g3, *refs):
    states, (out, buffer, done, turned, sems, out_sems) = refs[: 2 * len(BLOCKS)], refs[2 * len(BLOCKS) :]

    def place(k, half):
        layer, first = k // (NY // ROWS), pl.multiple_of(k % (NY // ROWS) * ROWS, ROWS)
        return (slice(None), layer, pl.ds(first, ROWS), pl.ds(half * 128, 128))

    def pieces(k, half):
        y, core = where[3] // 2, where[3] & 1
        copies = []
        for n, source in enumerate(states):
            step, first = BLOCKS[n % len(BLOCKS)]
            group = ((y + step) & 3) * 2 + (core if n < len(BLOCKS) else 1 - core)
            rows = pl.ds(group * MEM + first, source.shape[0])
            there = buffer.at[k, half, rows]
            copies.append(pltpu.make_async_copy(source.at[place(k, half)], there, sems.at[k, half, n]))
        return copies

    def result(k, half):
        return pltpu.make_async_copy(
            done.at[k, half], out.at[place(k, half)], out_sems.at[k, half]
        )

    @pl.loop(0, PIECES)
    def _(k):
        for half in range(HALVES):
            for copy in pieces(k, half):
                copy.start()

    sums = (g0[...] + g1[...]) + (g2[...] + g3[...])
    row = lax.broadcasted_iota(jnp.int32, (M, M), 0)
    column = lax.broadcasted_iota(jnp.int32, (M, M), 1)
    identity = jnp.where(row == column, 1.0, 0.0).astype(F32)
    scaled = identity + sums[0:M] / (M - 1)
    bound = jnp.max(jnp.sum(jnp.abs(scaled), axis=1, keepdims=True), axis=0, keepdims=True)
    root = scaled / bound
    inv_root = 1.5 * identity - 0.5 * root
    root = dot(root, inv_root)
    for step in range(1, NS_STEPS):
        factor = 1.5 * identity - 0.5 * dot(inv_root, root)
        if step < NS_STEPS - 1:
            root = dot(root, factor)
        inv_root = dot(factor, inv_root)
    contract = (((1,), (1,)), ((), ()))
    shift = sums[M : M + 8]
    for _ in range(2):
        shift = lax.dot_general(shift, inv_root, contract, precision=HIGH, preferred_element_type=F32)
    shift = shift[0:1] / bound / (M - 1)
    turned[...] = inv_root.T / jnp.sqrt(bound) + shift
    mine = turned[pl.ds(pl.multiple_of(where[3] * MEM, MEM), MEM), :]
    mine = mine + (1.0 - jnp.sum(mine, axis=1, keepdims=True)) * (1.0 / M)
    high = mine.astype(jnp.bfloat16)
    low = (mine - high.astype(F32)).astype(jnp.bfloat16)
    left = jnp.concatenate(
        [
            jnp.concatenate([high, high], axis=1),
            jnp.concatenate([low, jnp.zeros_like(low)], axis=1),
        ],
        axis=0,
    )

    @pl.loop(0, PIECES)
    def _(k):
        for half in range(HALVES):
            for copy in pieces(k, half):
                copy.wait()
        given = [buffer.at[k, half].reshape(M * ROWS, 128) for half in range(HALVES)]
        taken = [done.at[k, half].reshape(MEM * ROWS, 128) for half in range(HALVES)]
        for r in range(ROWS):
            state = jnp.concatenate([g[pl.ds(r, M, stride=ROWS), :] for g in given], axis=1)
            upper = state.astype(jnp.bfloat16)
            lower = (state - upper.astype(F32)).astype(jnp.bfloat16)
            both = jnp.dot(
                left, jnp.concatenate([upper, lower], axis=0), preferred_element_type=F32
            )
            both = both[:MEM] + both[MEM:]
            for half in range(HALVES):
                taken[half][pl.ds(r, MEM, stride=ROWS), :] = both[:, half * 128 : half * 128 + 128]
        for half in range(HALVES):
            result(k, half).start()

    for k in range(PIECES):
        for half in range(HALVES):
            result(k, half).wait()


BIG = SUB * DEPTH * NY * NW
PARTS = shape(NZ, SUB, LAY, NY, NW)
PRED = shape(NZ, CHUNK // 128, SUB, 128)
PRESSED = pltpu.VMEM((SUB, HALVES, DEPTH, NY, 128), F32)
FOUND = pltpu.VMEM((SUB, 128, 128), F32)


def sweep(*ins):
    return call(
        sweeps_kernel,
        [PARTS, PRED],
        ins,
        [SM] * 3 + [VM] * 4,
        [HBM, VM],
        [pltpu.VMEM((ROOM, NY, NW), F32)] * 8
        + [pltpu.VMEM((NW, NW), jnp.bfloat16), PRESSED, FOUND]
        + [pltpu.SemaphoreType.DMA((SUB, HALVES, NZ))],
        64 * BIG,
        16 * BIG,
    )


def analyse(where, sums, states):
    return call(
        analysis_kernel,
        shape(MEM, LAY, NY, NW),
        [where, *sums, *states],
        [SM] + [VM] * NX + [HBM] * (2 * len(BLOCKS)),
        ANY,
        [
            pltpu.VMEM((PIECES, HALVES, M, ROWS, 128), F32),
            pltpu.VMEM((PIECES, HALVES, MEM, ROWS, 128), F32),
            pltpu.VMEM((M, M), F32),
            pltpu.SemaphoreType.DMA((PIECES, HALVES, 2 * len(BLOCKS))),
            pltpu.SemaphoreType.DMA((PIECES, HALVES)),
        ],
        2 * M * MEM * LAY * NY * NW,
        4 * M * LAY * NY * NW,
    )


def shift_from(array, axis, size, by):
    return lax.ppermute(array, axis, [((i + by) % size, i) for i in range(size)])


def exchange(copies, axis):
    return lax.all_to_all(copies, axis, 0, 0, tiled=True)


def strip_kernel(mem, source, out, sems):
    copies = []
    for slab in range(NZ):
        rows = source.at[:, pl.ds(pl.multiple_of(mem[0] * ROWS_OF, ROWS_OF), ROWS_OF)]
        copies.append(pltpu.make_async_copy(rows, out.at[slab], sems.at[slab]))
    for copy in copies:
        copy.start()
    for copy in copies:
        copy.wait()


def strips_kernel(strips, out):
    for copy in range(NMEM):
        for slab in range(NZ):
            out[copy, LAY * slab : LAY * slab + LAY] = strips[slab]


def preds_kernel(parts, out):
    for g in range(NZ):
        for m in range(SUB):
            for k in range(CHUNK // 128):
                row = g * SUB + m
                out[k, row : row + 1, :] = parts[g, k, m : m + 1, :]


def group_at(mem, e):
    return (((mem // 2 + e // 2) & (NMEM // 2 - 1)) * 2) + ((mem & 1) ^ (e & 1))


def round_mem(array):
    parts = [array]
    for e in range(1, NMEM):
        pairs = [(group_at(i, e), i) for i in range(NMEM)]
        parts.append(lax.ppermute(array, ("y", "core"), pairs))
    return parts


def to_mem(kernel, parts, dims):
    copies = call(kernel, shape(NMEM, *dims), [parts], [VM], VM, [], 2**20, 2**20)
    return exchange(copies, ("y", "core"))


def body(logperm, source, obs_cells, obs_values, obs_prec):
    x, z, mem = lax.axis_index("x"), lax.axis_index("z"), lax.axis_index(("y", "core"))

    def swapped(array):
        return lax.ppermute(array, "core", [(0, 1), (1, 0)])

    half = MEM // 2
    after, before = shift_from(logperm, "y", 4, 1), shift_from(logperm, "y", 4, 3)
    far_a, far_b = shift_from(after[:half], "y", 4, 1), shift_from(before[half:], "y", 4, 3)
    others = [swapped(array) for array in (logperm, after, before)]
    others += [swapped(array) for array in (far_a, far_b)]
    states = [logperm, after, before, far_a, far_b, *others]

    strip = call(
        strip_kernel,
        shape(NZ, LAY, ROWS_OF, NW),
        [jnp.reshape(mem, (1,)).astype(jnp.int32), source],
        [SM, VM],
        HBM,
        [pltpu.SemaphoreType.DMA((NZ,))],
        2**20,
        2**20,
    )
    strips = exchange(strip, "z")

    def members_of(group):
        start = ((group & (NZ - 1)) * SUB, 0, 0, 0)
        sizes = (SUB, LAY, NY, NW)
        return lax.dynamic_slice(logperm, start, sizes, allow_negative_indices=False)

    parts = [members_of(z)] + [None] * (NZ - 1)
    for d in (4, 1, 7, 2, 6, 3, 5):
        parts[d] = shift_from(members_of(z - d), "z", NZ, d)
    sources = to_mem(strips_kernel, strips, (DEPTH, ROWS_OF, NW))

    cells, prec, values = lax.sort((obs_cells, obs_prec, obs_values), num_keys=1)
    block = lax.shift_right_logical(cells, BLOCK_BITS)
    counts = jnp.sum(block[None, :] == jnp.arange(NX)[:, None], axis=1).astype(jnp.int32)
    begin = jnp.sum(jnp.where(jnp.arange(NX) < x, counts, 0))
    count = jnp.sum(jnp.where(jnp.arange(NX) == x, counts, 0))
    most = jnp.max(counts)

    def window(done):
        want = jnp.minimum(begin + done, begin + count)
        first = jnp.minimum(want, NOBS - CHUNK)
        stop = jnp.minimum(want + CHUNK, begin + count)
        where = jnp.stack([z, want - first, jnp.maximum(stop - first, 0), mem]).astype(jnp.int32)

        def cut(array):
            return lax.dynamic_slice(array, (first,), (CHUNK,), allow_negative_indices=False)

        at = cut(cells)
        half = lax.shift_right_logical(at, 7) & (HALVES - 1)
        spots = half * (DEPTH * NY) + (lax.shift_right_logical(at, 8) & (DEPTH * NY - 1))
        place = jnp.arange(CHUNK, dtype=jnp.int32)
        lanes = jnp.where((place >= where[1]) & (place < where[2]), at & 127, -1)
        return where, spots, lanes, cut(prec)[None], cut(values)[None]

    where, spots_0, lanes_0, prec_0, values_0 = window(0)
    edge = shape(SUB, HALO, NY, NW)
    h, first, last = call(
        roots_kernel,
        [shape(SUB, DEPTH, NY, NW), edge, edge],
        [jnp.reshape(z, (1,)).astype(jnp.int32), *parts],
        [SM] + [HBM] * NZ,
        [VM] * 3,
        [pltpu.VMEM((NZ, SUB, LAY, NY, NW), F32), pltpu.SemaphoreType.DMA((NZ,))],
        4 * BIG,
        12 * BIG,
    )
    up = [(i, i + 1) for i in range(NX - 1)]
    down = [(i + 1, i) for i in range(NX - 1)]
    h_left, h_right = lax.ppermute(last, "x", up), lax.ppermute(first, "x", down)
    s_left = lax.ppermute(sources[:, DEPTH - HALO :], "x", up)
    s_right = lax.ppermute(sources[:, :HALO], "x", down)

    spare = jnp.zeros((NMEM, 2, ROWS_OF, NW), F32)
    sources = jnp.concatenate([s_left, sources, s_right, spare], axis=1)
    sent, pred = sweep(where, spots_0, lanes_0, h, h_left, h_right, sources)

    def group_preds(parts):
        dims = (CHUNK // 128, MEM, 128)
        return call(preds_kernel, shape(*dims), [parts], [VM], VM, [], 2**20, 2**20)

    def gram_of(first, parts, prec_cut, value_cut):
        return call(
            gram_kernel,
            shape(M + 8, M),
            [jnp.reshape(first, (1,)).astype(jnp.int32), *parts, prec_cut, value_cut],
            [SM] + [VM] * (NMEM + 2),
            VM,
            [pltpu.VMEM((NMEM, CHUNK // 128, MEM, 128), F32)],
            2 * M * M * CHUNK,
            4 * M * CHUNK,
        )

    def more(carry):
        done, total = carry
        where_n, spots_n, lanes_n, prec_n, values_n = window(done)
        pred_n = call(
            more_kernel,
            PRED,
            [where_n, spots_n, lanes_n, sent],
            [SM] * 3 + [VM],
            VM,
            [PRESSED, FOUND],
            BIG,
            8 * BIG,
        )
        group = group_preds(lax.all_gather(pred_n[0], "z"))
        groups = lax.all_gather(group, ("y", "core"))
        split = [groups[g] for g in range(NMEM)]
        return done + CHUNK, total + gram_of(jnp.int32(0), split, prec_n, values_n)

    gathered = exchange(pred, "z")
    groups = round_mem(group_preds(gathered))
    total = gram_of(mem, groups, prec_0, values_0)
    pressure = exchange(sent.reshape(MEM, LAY, NY, NW), "z")
    _, total = lax.while_loop(lambda c: c[0] < most, more, (jnp.int32(CHUNK), total))
    others = [shift_from(total, "x", NX, d) for d in range(1, NX)]

    analysis = analyse(where, [total, *others], states)
    return pressure, analysis


def solution(mesh):
    fine = Mesh(mesh.devices.reshape(NX, NZ, NMEM // 2, 2), ("x", "z", "y", "core"))
    cell, mem = ("x", "z"), ("y", "core")
    return jax.shard_map(
        body,
        mesh=fine,
        in_specs=(P(mem, cell, None, None), P(cell, None, None), P(), P(), P()),
        out_specs=(P(mem, cell, None, None), P(mem, cell, None, None)),
        check_vma=False,
    )
```

```python
import jax
import jax.numpy as jnp
from jax import lax
from jax.experimental import pallas as pl
from jax.experimental.pallas import tpu as pltpu
from jax.sharding import Mesh
from jax.sharding import PartitionSpec as P

M = 128
NOBS = 4096
NS_STEPS = 10
CPRESS = 0.05
HIGH = lax.Precision.HIGHEST
F32 = jnp.float32

NX, NZ, NMEM = 4, 8, 8
LAY = 2
MEM = M // NMEM
SUB = MEM // NZ
DEPTH = NZ * LAY
HALO = 4
FULL = DEPTH + 2 * HALO
GROUP = 4
ROOM = FULL + 6
NY, NW = 64, 256
HALVES = NW // 128
ROWS_OF = NY // NMEM
CHUNK = 1280
BLOCK_BITS = 18

VM = pl.BlockSpec(memory_space=pltpu.VMEM)
SM = pl.BlockSpec(memory_space=pltpu.SMEM)
ANY = pl.BlockSpec(memory_space=pl.ANY)
HBM = pl.BlockSpec(memory_space=pltpu.HBM)


def shape(*dims):
    return jax.ShapeDtypeStruct(dims, F32)


LIMITS = {"roots": 16, "sweeps": 32, "analysis": 32, "more": 16}


def call(kernel, outs, ins, specs, out_specs, scratch, flops, moved, name):
    return pl.pallas_call(
        kernel,
        out_shape=outs,
        in_specs=specs,
        out_specs=out_specs,
        scratch_shapes=scratch,
        cost_estimate=pl.CostEstimate(flops=flops, bytes_accessed=moved, transcendentals=0),
        compiler_params=pltpu.CompilerParams(vmem_limit_bytes=LIMITS.get(name, 8) * 2**20),
    )(*ins)


def roots_kernel(where, *refs):
    parts, (h_ref, first_ref, last_ref, buffer, h, sems, out_sems) = refs[:NZ], refs[NZ:]
    copies = [pltpu.make_async_copy(parts[d], buffer.at[d], sems.at[d]) for d in range(NZ)]
    for copy in copies:
        copy.start()
    results = []
    for d in range(NZ):
        copies[d].wait()
        slab = (where[0] + d) & (NZ - 1)
        for m in range(SUB):
            for a in range(LAY):
                h[m, slab * LAY + a] = jnp.exp(0.5 * buffer[d, m, a])
        layers = pl.ds(slab * LAY, LAY)
        results.append(pltpu.make_async_copy(h.at[:, layers], h_ref.at[:, layers], out_sems.at[d]))
        results[-1].start()
    first_ref[...] = h[:, 0:HALO]
    last_ref[...] = h[:, DEPTH - HALO : DEPTH]
    for result in results:
        result.wait()


TILES = [(i, half) for i in range(NY // 8) for half in range(NW // 128)]


def tile(i, half):
    return pl.ds(8 * i, 8), pl.ds(128 * half, 128)


def lane_sums(q, j, band, sums):
    value = q[pl.ds(j, GROUP)].reshape(GROUP * NY, NW)
    high = value.astype(jnp.bfloat16)
    low = (value - high.astype(F32)).astype(jnp.bfloat16)
    both = jnp.dot(jnp.concatenate([high, low], axis=0), band[...], preferred_element_type=F32)
    both = both[: GROUP * NY] + both[GROUP * NY :]
    sums[pl.ds(j, GROUP)] = both.reshape(GROUP, NY, NW)


def near_sums(q, sums, j):
    row = lax.broadcasted_iota(jnp.int32, (8, 128), 0)
    middle = {t: q[(j, *tile(*t))] for t in TILES}
    below = {t: pltpu.roll(middle[t], 1, 0) for t in TILES}
    above = {t: pltpu.roll(middle[t], 7, 0) for t in TILES}
    total = {}
    for i, half in TILES:
        t = (i, half)
        side = jnp.where(row == 0, below.get((i - 1, half), 0.0), below[t])
        side = side + jnp.where(row == 7, above.get((i + 1, half), 0.0), above[t])
        side = side + sums[(j, *tile(*t))]
        total[t] = side + (q[(j - 1, *tile(*t))] + q[(j + 1, *tile(*t))])
    return middle, total


def over_layers(q, band, sums, first, groups, step):
    lane_sums(q, first, band, sums)

    @pl.loop(0, groups)
    def _(c):
        j = first + c * GROUP
        for k in range(GROUP):
            step(j + k)
        lane_sums(q, j + GROUP, band, sums)


def gather_all(where, spots, lanes, press, found, copies):
    out = copies.at[0]
    out[...] = jnp.zeros_like(out)
    low, high = where[1] // 128, (where[2] + 127) // 128
    lane = lax.broadcasted_iota(jnp.int32, (1, 128), 1)
    flat = [press.at[m].reshape(HALVES * DEPTH * NY, 128) for m in range(SUB)]

    @pl.loop(low, high)
    def _(k):
        def one(o, carry):
            at = k * 128 + o
            spot, wanted = spots[at], lanes[at]
            for m in range(SUB):
                row = flat[m][pl.ds(spot, 1), :]
                found[m, pl.ds(o, 1), :] = jnp.where(lane == wanted, row, 0.0)
            return carry

        lax.fori_loop(0, 128, one, 0, unroll=16)
        for m in range(SUB):
            out[k, m : m + 1, :] = jnp.sum(found[m].T, axis=0, keepdims=True)

    for copy in range(1, NZ):
        copies[copy] = out[...]


def sweeps_kernel(where, spots, lanes, h_ref, hl_ref, hr_ref, s_mid, sl_ref, sr_ref, *refs):
    out, pred_ref, h_all, s_ref, qs, qw, qb, qc, rest, weight, sums, band, *refs = refs
    press, found, sems, in_sems, s_sems = refs
    cuts = [(0, HALO), (HALO, DEPTH), (HALO + DEPTH, HALO)]

    def roots(m):
        copies = []
        for n, source in enumerate((hl_ref, h_ref, hr_ref)):
            first, layers = cuts[n]
            there = h_all.at[m, pl.ds(1 + first, layers)]
            copies.append(pltpu.make_async_copy(source.at[m], there, in_sems.at[m, n]))
        return copies

    strips = []
    for n, source in enumerate((sl_ref, s_mid, sr_ref)):
        there = s_ref.at[:, pl.ds(*cuts[n])]
        strips.append(pltpu.make_async_copy(source, there, s_sems.at[n]))
    for copy in [*roots(0), *strips, *roots(1)]:
        copy.start()

    def results(m):
        copies = []
        for slab in range(NZ):
            for half in range(HALVES):
                done = press.at[m, half, pl.ds(slab * LAY, LAY)]
                place = out.at[slab, m, :, :, pl.ds(128 * half, 128)]
                copies.append(pltpu.make_async_copy(done, place, sems.at[m, half, slab]))
        return copies

    row = lax.broadcasted_iota(jnp.int32, (NW, NW), 0)
    column = lax.broadcasted_iota(jnp.int32, (NW, NW), 1)
    band[...] = jnp.where(jnp.abs(row - column) == 1, 1.0, 0.0).astype(jnp.bfloat16)
    s_ref[:, FULL : FULL + 2] = jnp.zeros((NMEM, 2, ROWS_OF, NW), F32)
    for m in range(SUB):
        h_all[m, 0] = jnp.zeros((NY, NW), F32)
        h_all[m, FULL + 1 : ROOM] = jnp.zeros((ROOM - FULL - 1, NY, NW), F32)
    for copy in strips:
        copy.wait()

    @pl.loop(0, SUB)
    def _(m):
        for copy in roots(m):
            copy.wait()
        h = h_all.at[m]

        def prepare(j):
            root, near = near_sums(h, sums, j)
            for i, half in TILES:
                t, spot = (i, half), (j, *tile(i, half))
                inverse = 1.0 / (CPRESS + root[t] * near[t])
                start = s_ref[i, j - 1, :, pl.ds(128 * half, 128)] * inverse
                slope = root[t] * inverse
                rest[spot] = start
                weight[spot] = slope
                qs[spot] = root[t] * start
                qw[spot] = root[t] * slope

        def sweep_to(new, old):
            def step(j):
                _, near = near_sums(old, sums, j)
                for t in TILES:
                    spot = (j, *tile(*t))
                    new[spot] = qs[spot] + qw[spot] * near[t]

            return step

        def last(j):
            _, near = near_sums(qc, sums, j)
            for i, half in TILES:
                spot = (j, *tile(i, half))
                value = rest[spot] + weight[spot] * near[i, half]
                press[m, half, j - HALO - 1, pl.ds(8 * i, 8), :] = value

        over_layers(h, band, sums, 2, 6, prepare)
        over_layers(qs, band, sums, 3, 5, sweep_to(qb, qs))
        over_layers(qb, band, sums, 4, 5, sweep_to(qc, qb))
        over_layers(qc, band, sums, 5, 4, last)

        for copy in results(m):
            copy.start()

    gather_all(where, spots, lanes, press, found, pred_ref)

    @pl.loop(0, SUB)
    def _(m):
        for copy in results(m):
            copy.wait()


def more_kernel(where, spots, lanes, parts, pred_ref, press, found):
    for slab in range(NZ):
        for m in range(SUB):
            for half in range(HALVES):
                lanes_of = pl.ds(128 * half, 128)
                press[m, half, slab * LAY : slab * LAY + LAY] = parts[slab, m, :, :, lanes_of]
    gather_all(where, spots, lanes, press, found, pred_ref)


def gram_kernel(mem, *refs):
    parts, (prec_ref, value_ref, out_ref, preds) = refs[:NMEM], refs[NMEM:]
    for e in range(NMEM):
        preds[group_at(mem[0], e)] = parts[e][...]
    pred = jnp.concatenate([preds[:, k].reshape(M, 128) for k in range(CHUNK // 128)], axis=1)
    prec = prec_ref[...]
    mean = jnp.sum(pred, axis=0, keepdims=True) * (1.0 / M)
    anomaly = pred - mean
    contract = (((1,), (1,)), ((), ()))
    out_ref[0:M] = lax.dot_general(
        anomaly * prec, anomaly, contract, precision=HIGH, preferred_element_type=F32
    )
    misfit = jnp.broadcast_to(prec * (value_ref[...] - mean), (8, CHUNK))
    out_ref[M : M + 8] = lax.dot_general(
        misfit, anomaly, contract, precision=HIGH, preferred_element_type=F32
    )


def dot(a, b):
    return jnp.dot(a, b, precision=HIGH, preferred_element_type=F32)


PIECES = 8
ROWS = LAY * NY // PIECES


BLOCKS = [(0, 0), (1, 0), (3, 0), (2, 0), (2, MEM // 2)]


def analysis_kernel(where, g0, g1, g2, g3, *refs):
    states, (out, buffer, done, turned, sems, out_sems) = refs[: 2 * len(BLOCKS)], refs[2 * len(BLOCKS) :]

    def place(k, half):
        layer, first = k // (NY // ROWS), pl.multiple_of(k % (NY // ROWS) * ROWS, ROWS)
        return (slice(None), layer, pl.ds(first, ROWS), pl.ds(half * 128, 128))

    def pieces(k, half):
        y, core = where[3] // 2, where[3] & 1
        copies = []
        for n, source in enumerate(states):
            step, first = BLOCKS[n % len(BLOCKS)]
            group = ((y + step) & 3) * 2 + (core if n < len(BLOCKS) else 1 - core)
            rows = pl.ds(group * MEM + first, source.shape[0])
            there = buffer.at[k, half, rows]
            copies.append(pltpu.make_async_copy(source.at[place(k, half)], there, sems.at[k, half, n]))
        return copies

    def result(k, half):
        return pltpu.make_async_copy(
            done.at[k, half], out.at[place(k, half)], out_sems.at[k, half]
        )

    @pl.loop(0, PIECES)
    def _(k):
        for half in range(HALVES):
            for copy in pieces(k, half):
                copy.start()

    sums = (g0[...] + g1[...]) + (g2[...] + g3[...])
    row = lax.broadcasted_iota(jnp.int32, (M, M), 0)
    column = lax.broadcasted_iota(jnp.int32, (M, M), 1)
    identity = jnp.where(row == column, 1.0, 0.0).astype(F32)
    scaled = identity + sums[0:M] / (M - 1)
    bound = jnp.max(jnp.sum(jnp.abs(scaled), axis=1, keepdims=True), axis=0, keepdims=True)
    root = scaled / bound
    inv_root = 1.5 * identity - 0.5 * root
    root = dot(root, inv_root)
    for step in range(1, NS_STEPS):
        factor = 1.5 * identity - 0.5 * dot(inv_root, root)
        if step < NS_STEPS - 1:
            root = dot(root, factor)
        inv_root = dot(factor, inv_root)
    contract = (((1,), (1,)), ((), ()))
    shift = sums[M : M + 8]
    for _ in range(2):
        shift = lax.dot_general(shift, inv_root, contract, precision=HIGH, preferred_element_type=F32)
    shift = shift[0:1] / bound / (M - 1)
    turned[...] = inv_root.T / jnp.sqrt(bound) + shift
    mine = turned[pl.ds(pl.multiple_of(where[3] * MEM, MEM), MEM), :]
    mine = mine + (1.0 - jnp.sum(mine, axis=1, keepdims=True)) * (1.0 / M)
    high = mine.astype(jnp.bfloat16)
    low = (mine - high.astype(F32)).astype(jnp.bfloat16)
    left = jnp.concatenate(
        [
            jnp.concatenate([high, high], axis=1),
            jnp.concatenate([low, jnp.zeros_like(low)], axis=1),
        ],
        axis=0,
    )

    @pl.loop(0, PIECES)
    def _(k):
        for half in range(HALVES):
            for copy in pieces(k, half):
                copy.wait()
        given = [buffer.at[k, half].reshape(M * ROWS, 128) for half in range(HALVES)]
        taken = [done.at[k, half].reshape(MEM * ROWS, 128) for half in range(HALVES)]
        for r in range(ROWS):
            state = jnp.concatenate([g[pl.ds(r, M, stride=ROWS), :] for g in given], axis=1)
            upper = state.astype(jnp.bfloat16)
            lower = (state - upper.astype(F32)).astype(jnp.bfloat16)
            both = jnp.dot(
                left, jnp.concatenate([upper, lower], axis=0), preferred_element_type=F32
            )
            both = both[:MEM] + both[MEM:]
            for half in range(HALVES):
                taken[half][pl.ds(r, MEM, stride=ROWS), :] = both[:, half * 128 : half * 128 + 128]
        for half in range(HALVES):
            result(k, half).start()

    for k in range(PIECES):
        for half in range(HALVES):
            result(k, half).wait()


BIG = SUB * DEPTH * NY * NW
PARTS = shape(NZ, SUB, LAY, NY, NW)
PRED = shape(NZ, CHUNK // 128, SUB, 128)
PRESSED = pltpu.VMEM((SUB, HALVES, DEPTH, NY, 128), F32)
FOUND = pltpu.VMEM((SUB, 128, 128), F32)


def sweep(*ins):
    return call(
        sweeps_kernel,
        [PARTS, PRED],
        ins,
        [SM] * 3 + [HBM] + [ANY] * 5,
        [HBM, VM],
        [pltpu.VMEM((SUB, ROOM, NY, NW), F32), pltpu.VMEM((NMEM, FULL + 2, ROWS_OF, NW), F32)]
        + [pltpu.VMEM((ROOM, NY, NW), F32)] * 7
        + [pltpu.VMEM((NW, NW), jnp.bfloat16), PRESSED, FOUND]
        + [pltpu.SemaphoreType.DMA((SUB, HALVES, NZ))]
        + [pltpu.SemaphoreType.DMA((SUB, 3)), pltpu.SemaphoreType.DMA((3,))],
        64 * BIG,
        16 * BIG,
        "sweeps",
    )


def analyse(where, sums, states):
    return call(
        analysis_kernel,
        shape(MEM, LAY, NY, NW),
        [where, *sums, *states],
        [SM] + [VM] * NX + [HBM] * (2 * len(BLOCKS)),
        ANY,
        [
            pltpu.VMEM((PIECES, HALVES, M, ROWS, 128), F32),
            pltpu.VMEM((PIECES, HALVES, MEM, ROWS, 128), F32),
            pltpu.VMEM((M, M), F32),
            pltpu.SemaphoreType.DMA((PIECES, HALVES, 2 * len(BLOCKS))),
            pltpu.SemaphoreType.DMA((PIECES, HALVES)),
        ],
        2 * M * MEM * LAY * NY * NW,
        4 * M * LAY * NY * NW,
        "analysis",
    )


def shift_from(array, axis, size, by):
    return lax.ppermute(array, axis, [((i + by) % size, i) for i in range(size)])


def exchange(copies, axis):
    return lax.all_to_all(copies, axis, 0, 0, tiled=True)


def strip_kernel(mem, source, out, sems):
    copies = []
    for slab in range(NZ):
        rows = source.at[:, pl.ds(pl.multiple_of(mem[0] * ROWS_OF, ROWS_OF), ROWS_OF)]
        copies.append(pltpu.make_async_copy(rows, out.at[slab], sems.at[slab]))
    for copy in copies:
        copy.start()
    for copy in copies:
        copy.wait()


def strips_kernel(strips, out):
    for copy in range(NMEM):
        for slab in range(NZ):
            out[copy, LAY * slab : LAY * slab + LAY] = strips[slab]


def preds_kernel(parts, out):
    for g in range(NZ):
        for m in range(SUB):
            for k in range(CHUNK // 128):
                row = g * SUB + m
                out[k, row : row + 1, :] = parts[g, k, m : m + 1, :]


def group_at(mem, e):
    return (((mem // 2 + e // 2) & (NMEM // 2 - 1)) * 2) + ((mem & 1) ^ (e & 1))


def round_mem(array):
    parts = [array]
    for e in range(1, NMEM):
        pairs = [(group_at(i, e), i) for i in range(NMEM)]
        parts.append(lax.ppermute(array, ("y", "core"), pairs))
    return parts


def to_mem(kernel, parts, dims, name):
    copies = call(kernel, shape(NMEM, *dims), [parts], [VM], VM, [], 2**20, 2**20, name)
    return exchange(copies, ("y", "core"))


def body(logperm, source, obs_cells, obs_values, obs_prec):
    x, z, mem = lax.axis_index("x"), lax.axis_index("z"), lax.axis_index(("y", "core"))

    def swapped(array):
        return lax.ppermute(array, "core", [(0, 1), (1, 0)])

    half = MEM // 2
    after, before = shift_from(logperm, "y", 4, 1), shift_from(logperm, "y", 4, 3)
    far_a, far_b = shift_from(after[:half], "y", 4, 1), shift_from(before[half:], "y", 4, 3)
    others = [swapped(array) for array in (logperm, after, before)]
    others += [swapped(array) for array in (far_a, far_b)]
    states = [logperm, after, before, far_a, far_b, *others]

    strip = call(
        strip_kernel,
        pltpu.HBM((NZ, LAY, ROWS_OF, NW), F32),
        [jnp.reshape(mem, (1,)).astype(jnp.int32), source],
        [SM, VM],
        HBM,
        [pltpu.SemaphoreType.DMA((NZ,))],
        2**20,
        2**20,
        "strip",
    )
    strips = exchange(strip, "z")

    def members_of(group):
        start = ((group & (NZ - 1)) * SUB, 0, 0, 0)
        sizes = (SUB, LAY, NY, NW)
        return lax.dynamic_slice(logperm, start, sizes, allow_negative_indices=False)

    parts = [members_of(z)] + [None] * (NZ - 1)
    for d in (4, 1, 7, 2, 6, 3, 5):
        parts[d] = shift_from(members_of(z - d), "z", NZ, d)
    sources = to_mem(strips_kernel, strips, (DEPTH, ROWS_OF, NW), "strips")

    cells, prec, values = lax.sort((obs_cells, obs_prec, obs_values), num_keys=1)
    block = lax.shift_right_logical(cells, BLOCK_BITS)
    counts = jnp.sum(block[None, :] == jnp.arange(NX)[:, None], axis=1).astype(jnp.int32)
    begin = jnp.sum(jnp.where(jnp.arange(NX) < x, counts, 0))
    count = jnp.sum(jnp.where(jnp.arange(NX) == x, counts, 0))
    most = jnp.max(counts)

    def window(done):
        want = jnp.minimum(begin + done, begin + count)
        first = jnp.minimum(want, NOBS - CHUNK)
        stop = jnp.minimum(want + CHUNK, begin + count)
        where = jnp.stack([z, want - first, jnp.maximum(stop - first, 0), mem]).astype(jnp.int32)

        def cut(array):
            return lax.dynamic_slice(array, (first,), (CHUNK,), allow_negative_indices=False)

        at = cut(cells)
        half = lax.shift_right_logical(at, 7) & (HALVES - 1)
        spots = half * (DEPTH * NY) + (lax.shift_right_logical(at, 8) & (DEPTH * NY - 1))
        place = jnp.arange(CHUNK, dtype=jnp.int32)
        lanes = jnp.where((place >= where[1]) & (place < where[2]), at & 127, -1)
        return where, spots, lanes, cut(prec)[None], cut(values)[None]

    where, spots_0, lanes_0, prec_0, values_0 = window(0)
    edge = shape(SUB, HALO, NY, NW)
    h, first, last = call(
        roots_kernel,
        [pltpu.HBM((SUB, DEPTH, NY, NW), F32), edge, edge],
        [jnp.reshape(z, (1,)).astype(jnp.int32), *parts],
        [SM] + [ANY] * NZ,
        [HBM, VM, VM],
        [
            pltpu.VMEM((NZ, SUB, LAY, NY, NW), F32),
            pltpu.VMEM((SUB, DEPTH, NY, NW), F32),
            pltpu.SemaphoreType.DMA((NZ,)),
            pltpu.SemaphoreType.DMA((NZ,)),
        ],
        4 * BIG,
        12 * BIG,
        "roots",
    )
    up = [(i, i + 1) for i in range(NX - 1)]
    down = [(i + 1, i) for i in range(NX - 1)]
    h_left, h_right = lax.ppermute(last, "x", up), lax.ppermute(first, "x", down)
    s_left = lax.ppermute(sources[:, DEPTH - HALO :], "x", up)
    s_right = lax.ppermute(sources[:, :HALO], "x", down)

    sent, pred = sweep(where, spots_0, lanes_0, h, h_left, h_right, sources, s_left, s_right)

    def group_preds(parts):
        dims = (CHUNK // 128, MEM, 128)
        return call(preds_kernel, shape(*dims), [parts], [VM], VM, [], 2**20, 2**20, "preds")

    def gram_of(first, parts, prec_cut, value_cut):
        return call(
            gram_kernel,
            shape(M + 8, M),
            [jnp.reshape(first, (1,)).astype(jnp.int32), *parts, prec_cut, value_cut],
            [SM] + [VM] * (NMEM + 2),
            VM,
            [pltpu.VMEM((NMEM, CHUNK // 128, MEM, 128), F32)],
            2 * M * M * CHUNK,
            4 * M * CHUNK,
            "gram",
        )

    def more(carry):
        done, total = carry
        where_n, spots_n, lanes_n, prec_n, values_n = window(done)
        pred_n = call(
            more_kernel,
            PRED,
            [where_n, spots_n, lanes_n, sent],
            [SM] * 3 + [VM],
            VM,
            [PRESSED, FOUND],
            BIG,
            8 * BIG,
            "more",
        )
        group = group_preds(lax.all_gather(pred_n[0], "z"))
        groups = lax.all_gather(group, ("y", "core"))
        split = [groups[g] for g in range(NMEM)]
        return done + CHUNK, total + gram_of(jnp.int32(0), split, prec_n, values_n)

    gathered = exchange(pred, "z")
    groups = round_mem(group_preds(gathered))
    total = gram_of(mem, groups, prec_0, values_0)
    pressure = exchange(sent.reshape(MEM, LAY, NY, NW), "z")
    _, total = lax.while_loop(lambda c: c[0] < most, more, (jnp.int32(CHUNK), total))
    others = [shift_from(total, "x", NX, d) for d in range(1, NX)]

    analysis = analyse(where, [total, *others], states)
    return pressure, analysis


def solution(mesh):
    fine = Mesh(mesh.devices.reshape(NX, NZ, NMEM // 2, 2), ("x", "z", "y", "core"))
    cell, mem = ("x", "z"), ("y", "core")
    return jax.shard_map(
        body,
        mesh=fine,
        in_specs=(P(mem, cell, None, None), P(cell, None, None), P(), P(), P()),
        out_specs=(P(mem, cell, None, None), P(mem, cell, None, None)),
        check_vma=False,
    )
```

```python
import jax
import jax.numpy as jnp
from jax import lax
from jax.experimental import pallas as pl
from jax.experimental.pallas import tpu as pltpu
from jax.sharding import Mesh
from jax.sharding import PartitionSpec as P

M = 128
NOBS = 4096
NS_STEPS = 10
CPRESS = 0.05
HIGH = lax.Precision.HIGHEST
F32 = jnp.float32

NX, NZ, NMEM = 4, 8, 8
LAY = 2
MEM = M // NMEM
SUB = MEM // NZ
DEPTH = NZ * LAY
HALO = 4
FULL = DEPTH + 2 * HALO
GROUP = 4
ROOM = FULL + 6
NY, NW = 64, 256
HALVES = NW // 128
ROWS_OF = NY // NMEM
CHUNK = 1280
BLOCK_BITS = 18

VM = pl.BlockSpec(memory_space=pltpu.VMEM)
SM = pl.BlockSpec(memory_space=pltpu.SMEM)
ANY = pl.BlockSpec(memory_space=pl.ANY)
HBM = pl.BlockSpec(memory_space=pltpu.HBM)


def shape(*dims):
    return jax.ShapeDtypeStruct(dims, F32)


LIMITS = {"ends": 8, "sweeps": 32, "analysis": 32, "more": 16}


def call(kernel, outs, ins, specs, out_specs, scratch, flops, moved, name):
    return pl.pallas_call(
        kernel,
        out_shape=outs,
        in_specs=specs,
        out_specs=out_specs,
        scratch_shapes=scratch,
        cost_estimate=pl.CostEstimate(flops=flops, bytes_accessed=moved, transcendentals=0),
        compiler_params=pltpu.CompilerParams(vmem_limit_bytes=LIMITS.get(name, 8) * 2**20),
    )(*ins)


def root(value):
    return jnp.exp(0.5 * value)


def edges_kernel(where, *refs):
    parts, (first_ref, last_ref, buffer, sems) = refs[:NZ], refs[NZ:]
    ends = HALO // LAY

    def for_ends(act):
        for d in range(NZ):
            slab = (where[0] + d) & (NZ - 1)
            spot = jnp.where(slab < ends, slab, slab - (NZ - 2 * ends))

            @pl.when((slab < ends) | (slab >= NZ - ends))
            def _():
                act(pltpu.make_async_copy(parts[d], buffer.at[spot], sems.at[spot]))

    for_ends(lambda copy: copy.start())
    for_ends(lambda copy: copy.wait())
    for spot in range(ends):
        for m in range(SUB):
            layers = pl.ds(spot * LAY, LAY)
            first_ref[m, layers] = root(buffer[spot, m])
            last_ref[m, layers] = root(buffer[ends + spot, m])


TILES = [(i, half) for i in range(NY // 8) for half in range(NW // 128)]


def tile(i, half):
    return pl.ds(8 * i, 8), pl.ds(128 * half, 128)


def lane_sums(q, j, band, sums):
    value = q[pl.ds(j, GROUP)].reshape(GROUP * NY, NW)
    high = value.astype(jnp.bfloat16)
    low = (value - high.astype(F32)).astype(jnp.bfloat16)
    both = jnp.dot(jnp.concatenate([high, low], axis=0), band[...], preferred_element_type=F32)
    both = both[: GROUP * NY] + both[GROUP * NY :]
    sums[pl.ds(j, GROUP)] = both.reshape(GROUP, NY, NW)


def near_sums(q, sums, j):
    row = lax.broadcasted_iota(jnp.int32, (8, 128), 0)
    middle = {t: q[(j, *tile(*t))] for t in TILES}
    below = {t: pltpu.roll(middle[t], 1, 0) for t in TILES}
    above = {t: pltpu.roll(middle[t], 7, 0) for t in TILES}
    total = {}
    for i, half in TILES:
        t = (i, half)
        side = jnp.where(row == 0, below.get((i - 1, half), 0.0), below[t])
        side = side + jnp.where(row == 7, above.get((i + 1, half), 0.0), above[t])
        side = side + sums[(j, *tile(*t))]
        total[t] = side + (q[(j - 1, *tile(*t))] + q[(j + 1, *tile(*t))])
    return middle, total


def over_layers(q, band, sums, first, groups, step):
    lane_sums(q, first, band, sums)

    @pl.loop(0, groups)
    def _(c):
        j = first + c * GROUP
        for k in range(GROUP):
            step(j + k)
        lane_sums(q, j + GROUP, band, sums)


def gather_all(where, spots, lanes, press, found, copies):
    out = copies.at[0]
    out[...] = jnp.zeros_like(out)
    low, high = where[1] // 128, (where[2] + 127) // 128
    lane = lax.broadcasted_iota(jnp.int32, (1, 128), 1)
    flat = [press.at[m].reshape(HALVES * DEPTH * NY, 128) for m in range(SUB)]

    @pl.loop(low, high)
    def _(k):
        def one(o, carry):
            at = k * 128 + o
            spot, wanted = spots[at], lanes[at]
            for m in range(SUB):
                row = flat[m][pl.ds(spot, 1), :]
                found[m, pl.ds(o, 1), :] = jnp.where(lane == wanted, row, 0.0)
            return carry

        lax.fori_loop(0, 128, one, 0, unroll=16)
        for m in range(SUB):
            out[k, m : m + 1, :] = jnp.sum(found[m].T, axis=0, keepdims=True)

    for copy in range(1, NZ):
        copies[copy] = out[...]


def sweeps_kernel(where, spots, lanes, hl_ref, hr_ref, s_mid, sl_ref, sr_ref, *refs):
    parts, refs = refs[:NZ], refs[NZ:]
    out, pred_ref, h_all, raw, s_ref, qs, qw, qb, qc, rest, weight, sums, band, *refs = refs
    press, found, sems, in_sems, h_sems, s_sems = refs
    cuts = [(0, HALO), (HALO, DEPTH), (HALO + DEPTH, HALO)]

    halos = []
    for n, source in enumerate((hl_ref, hr_ref)):
        there = h_all.at[:, pl.ds(1 + cuts[2 * n][0], HALO)]
        halos.append(pltpu.make_async_copy(source, there, h_sems.at[n]))
    arrivals = [pltpu.make_async_copy(parts[d], raw.at[d], in_sems.at[d]) for d in range(NZ)]

    strips = []
    for n, source in enumerate((sl_ref, s_mid, sr_ref)):
        there = s_ref.at[:, pl.ds(*cuts[n])]
        strips.append(pltpu.make_async_copy(source, there, s_sems.at[n]))
    for copy in [*arrivals, *halos, *strips]:
        copy.start()

    def results(m):
        copies = []
        for slab in range(NZ):
            for half in range(HALVES):
                done = press.at[m, half, pl.ds(slab * LAY, LAY)]
                place = out.at[slab, m, :, :, pl.ds(128 * half, 128)]
                copies.append(pltpu.make_async_copy(done, place, sems.at[m, half, slab]))
        return copies

    row = lax.broadcasted_iota(jnp.int32, (NW, NW), 0)
    column = lax.broadcasted_iota(jnp.int32, (NW, NW), 1)
    band[...] = jnp.where(jnp.abs(row - column) == 1, 1.0, 0.0).astype(jnp.bfloat16)
    s_ref[:, FULL : FULL + 2] = jnp.zeros((NMEM, 2, ROWS_OF, NW), F32)
    for m in range(SUB):
        h_all[m, 0] = jnp.zeros((NY, NW), F32)
        h_all[m, FULL + 1 : ROOM] = jnp.zeros((ROOM - FULL - 1, NY, NW), F32)
    for copy in [*arrivals, *halos, *strips]:
        copy.wait()

    @pl.loop(0, SUB)
    def _(m):
        h = h_all.at[m]

        @pl.loop(0, NZ)
        def _(d):
            slab = (where[0] + d) & (NZ - 1)
            for a in range(LAY):
                h[1 + HALO + slab * LAY + a] = root(raw[d, m, a])

        def prepare(j):
            roots, near = near_sums(h, sums, j)
            for i, half in TILES:
                t, spot = (i, half), (j, *tile(i, half))
                inverse = 1.0 / (CPRESS + roots[t] * near[t])
                start = s_ref[i, j - 1, :, pl.ds(128 * half, 128)] * inverse
                slope = roots[t] * inverse
                rest[spot] = start
                weight[spot] = slope
                qs[spot] = roots[t] * start
                qw[spot] = roots[t] * slope

        def sweep_to(new, old):
            def step(j):
                _, near = near_sums(old, sums, j)
                for t in TILES:
                    spot = (j, *tile(*t))
                    new[spot] = qs[spot] + qw[spot] * near[t]

            return step

        def last(j):
            _, near = near_sums(qc, sums, j)
            for i, half in TILES:
                spot = (j, *tile(i, half))
                value = rest[spot] + weight[spot] * near[i, half]
                press[m, half, j - HALO - 1, pl.ds(8 * i, 8), :] = value

        over_layers(h, band, sums, 2, 6, prepare)
        over_layers(qs, band, sums, 3, 5, sweep_to(qb, qs))
        over_layers(qb, band, sums, 4, 5, sweep_to(qc, qb))
        over_layers(qc, band, sums, 5, 4, last)

        for copy in results(m):
            copy.start()

    gather_all(where, spots, lanes, press, found, pred_ref)

    @pl.loop(0, SUB)
    def _(m):
        for copy in results(m):
            copy.wait()


def more_kernel(where, spots, lanes, parts, pred_ref, press, found):
    for slab in range(NZ):
        for m in range(SUB):
            for half in range(HALVES):
                lanes_of = pl.ds(128 * half, 128)
                press[m, half, slab * LAY : slab * LAY + LAY] = parts[slab, m, :, :, lanes_of]
    gather_all(where, spots, lanes, press, found, pred_ref)


def gram_kernel(mem, *refs):
    parts, (prec_ref, value_ref, out_ref, preds) = refs[:NMEM], refs[NMEM:]
    for e in range(NMEM):
        preds[group_at(mem[0], e)] = parts[e][...]
    pred = jnp.concatenate([preds[:, k].reshape(M, 128) for k in range(CHUNK // 128)], axis=1)
    prec = prec_ref[...]
    mean = jnp.sum(pred, axis=0, keepdims=True) * (1.0 / M)
    anomaly = pred - mean
    contract = (((1,), (1,)), ((), ()))
    out_ref[0:M] = lax.dot_general(
        anomaly * prec, anomaly, contract, precision=HIGH, preferred_element_type=F32
    )
    misfit = jnp.broadcast_to(prec * (value_ref[...] - mean), (8, CHUNK))
    out_ref[M : M + 8] = lax.dot_general(
        misfit, anomaly, contract, precision=HIGH, preferred_element_type=F32
    )


def dot(a, b):
    return jnp.dot(a, b, precision=HIGH, preferred_element_type=F32)


PIECES = 8
ROWS = LAY * NY // PIECES


BLOCKS = [(0, 0), (1, 0), (3, 0), (2, 0), (2, MEM // 2)]


def analysis_kernel(where, g0, g1, g2, g3, *refs):
    states, (out, buffer, done, turned, sems, out_sems) = refs[: 2 * len(BLOCKS)], refs[2 * len(BLOCKS) :]

    def place(k, half):
        layer, first = k // (NY // ROWS), pl.multiple_of(k % (NY // ROWS) * ROWS, ROWS)
        return (slice(None), layer, pl.ds(first, ROWS), pl.ds(half * 128, 128))

    def pieces(k, half):
        y, core = where[3] // 2, where[3] & 1
        copies = []
        for n, source in enumerate(states):
            step, first = BLOCKS[n % len(BLOCKS)]
            group = ((y + step) & 3) * 2 + (core if n < len(BLOCKS) else 1 - core)
            rows = pl.ds(group * MEM + first, source.shape[0])
            there = buffer.at[k, half, rows]
            copies.append(pltpu.make_async_copy(source.at[place(k, half)], there, sems.at[k, half, n]))
        return copies

    def result(k, half):
        return pltpu.make_async_copy(
            done.at[k, half], out.at[place(k, half)], out_sems.at[k, half]
        )

    @pl.loop(0, PIECES)
    def _(k):
        for half in range(HALVES):
            for copy in pieces(k, half):
                copy.start()

    sums = (g0[...] + g1[...]) + (g2[...] + g3[...])
    row = lax.broadcasted_iota(jnp.int32, (M, M), 0)
    column = lax.broadcasted_iota(jnp.int32, (M, M), 1)
    identity = jnp.where(row == column, 1.0, 0.0).astype(F32)
    scaled = identity + sums[0:M] / (M - 1)
    bound = jnp.max(jnp.sum(jnp.abs(scaled), axis=1, keepdims=True), axis=0, keepdims=True)
    root = scaled / bound
    inv_root = 1.5 * identity - 0.5 * root
    root = dot(root, inv_root)
    for step in range(1, NS_STEPS):
        factor = 1.5 * identity - 0.5 * dot(inv_root, root)
        if step < NS_STEPS - 1:
            root = dot(root, factor)
        inv_root = dot(factor, inv_root)
    contract = (((1,), (1,)), ((), ()))
    shift = sums[M : M + 8]
    for _ in range(2):
        shift = lax.dot_general(shift, inv_root, contract, precision=HIGH, preferred_element_type=F32)
    shift = shift[0:1] / bound / (M - 1)
    turned[...] = inv_root.T / jnp.sqrt(bound) + shift
    mine = turned[pl.ds(pl.multiple_of(where[3] * MEM, MEM), MEM), :]
    mine = mine + (1.0 - jnp.sum(mine, axis=1, keepdims=True)) * (1.0 / M)
    high = mine.astype(jnp.bfloat16)
    low = (mine - high.astype(F32)).astype(jnp.bfloat16)
    left = jnp.concatenate(
        [
            jnp.concatenate([high, high], axis=1),
            jnp.concatenate([low, jnp.zeros_like(low)], axis=1),
        ],
        axis=0,
    )

    @pl.loop(0, PIECES)
    def _(k):
        for half in range(HALVES):
            for copy in pieces(k, half):
                copy.wait()
        given = [buffer.at[k, half].reshape(M * ROWS, 128) for half in range(HALVES)]
        taken = [done.at[k, half].reshape(MEM * ROWS, 128) for half in range(HALVES)]
        for r in range(ROWS):
            state = jnp.concatenate([g[pl.ds(r, M, stride=ROWS), :] for g in given], axis=1)
            upper = state.astype(jnp.bfloat16)
            lower = (state - upper.astype(F32)).astype(jnp.bfloat16)
            both = jnp.dot(
                left, jnp.concatenate([upper, lower], axis=0), preferred_element_type=F32
            )
            both = both[:MEM] + both[MEM:]
            for half in range(HALVES):
                taken[half][pl.ds(r, MEM, stride=ROWS), :] = both[:, half * 128 : half * 128 + 128]
        for half in range(HALVES):
            result(k, half).start()

    for k in range(PIECES):
        for half in range(HALVES):
            result(k, half).wait()


BIG = SUB * DEPTH * NY * NW
PARTS = shape(NZ, SUB, LAY, NY, NW)
PRED = shape(NZ, CHUNK // 128, SUB, 128)
PRESSED = pltpu.VMEM((SUB, HALVES, DEPTH, NY, 128), F32)
FOUND = pltpu.VMEM((SUB, 128, 128), F32)


def sweep(*ins):
    return call(
        sweeps_kernel,
        [PARTS, PRED],
        ins,
        [SM] * 3 + [ANY] * (5 + NZ),
        [HBM, VM],
        [pltpu.VMEM((SUB, ROOM, NY, NW), F32), pltpu.VMEM((NZ, SUB, LAY, NY, NW), F32)]
        + [pltpu.VMEM((NMEM, FULL + 2, ROWS_OF, NW), F32)]
        + [pltpu.VMEM((ROOM, NY, NW), F32)] * 7
        + [pltpu.VMEM((NW, NW), jnp.bfloat16), PRESSED, FOUND]
        + [pltpu.SemaphoreType.DMA((SUB, HALVES, NZ))]
        + [pltpu.SemaphoreType.DMA((n,)) for n in (NZ, 2, 3)],
        64 * BIG,
        16 * BIG,
        "sweeps",
    )


def analyse(where, sums, states):
    return call(
        analysis_kernel,
        shape(MEM, LAY, NY, NW),
        [where, *sums, *states],
        [SM] + [VM] * NX + [HBM] * (2 * len(BLOCKS)),
        ANY,
        [
            pltpu.VMEM((PIECES, HALVES, M, ROWS, 128), F32),
            pltpu.VMEM((PIECES, HALVES, MEM, ROWS, 128), F32),
            pltpu.VMEM((M, M), F32),
            pltpu.SemaphoreType.DMA((PIECES, HALVES, 2 * len(BLOCKS))),
            pltpu.SemaphoreType.DMA((PIECES, HALVES)),
        ],
        2 * M * MEM * LAY * NY * NW,
        4 * M * LAY * NY * NW,
        "analysis",
    )


def shift_from(array, axis, size, by):
    return lax.ppermute(array, axis, [((i + by) % size, i) for i in range(size)])


def exchange(copies, axis):
    return lax.all_to_all(copies, axis, 0, 0, tiled=True)


def strip_kernel(mem, source, out, sems):
    copies = []
    for slab in range(NZ):
        rows = source.at[:, pl.ds(pl.multiple_of(mem[0] * ROWS_OF, ROWS_OF), ROWS_OF)]
        copies.append(pltpu.make_async_copy(rows, out.at[slab], sems.at[slab]))
    for copy in copies:
        copy.start()
    for copy in copies:
        copy.wait()


def strips_kernel(strips, out):
    for copy in range(NMEM):
        for slab in range(NZ):
            out[copy, LAY * slab : LAY * slab + LAY] = strips[slab]


def preds_kernel(parts, out):
    for g in range(NZ):
        for m in range(SUB):
            for k in range(CHUNK // 128):
                row = g * SUB + m
                out[k, row : row + 1, :] = parts[g, k, m : m + 1, :]


def group_at(mem, e):
    return (((mem // 2 + e // 2) & (NMEM // 2 - 1)) * 2) + ((mem & 1) ^ (e & 1))


def round_mem(array):
    parts = [array]
    for e in range(1, NMEM):
        pairs = [(group_at(i, e), i) for i in range(NMEM)]
        parts.append(lax.ppermute(array, ("y", "core"), pairs))
    return parts


def to_mem(kernel, parts, dims, name):
    copies = call(kernel, shape(NMEM, *dims), [parts], [VM], VM, [], 2**20, 2**20, name)
    return exchange(copies, ("y", "core"))


def body(logperm, source, obs_cells, obs_values, obs_prec):
    x, z, mem = lax.axis_index("x"), lax.axis_index("z"), lax.axis_index(("y", "core"))

    def swapped(array):
        return lax.ppermute(array, "core", [(0, 1), (1, 0)])

    half = MEM // 2
    after, before = shift_from(logperm, "y", 4, 1), shift_from(logperm, "y", 4, 3)
    far_a, far_b = shift_from(after[:half], "y", 4, 1), shift_from(before[half:], "y", 4, 3)
    others = [swapped(array) for array in (logperm, after, before)]
    others += [swapped(array) for array in (far_a, far_b)]
    states = [logperm, after, before, far_a, far_b, *others]

    strip = call(
        strip_kernel,
        pltpu.HBM((NZ, LAY, ROWS_OF, NW), F32),
        [jnp.reshape(mem, (1,)).astype(jnp.int32), source],
        [SM, VM],
        HBM,
        [pltpu.SemaphoreType.DMA((NZ,))],
        2**20,
        2**20,
        "strip",
    )
    strips = exchange(strip, "z")

    def members_of(group):
        start = ((group & (NZ - 1)) * SUB, 0, 0, 0)
        sizes = (SUB, LAY, NY, NW)
        return lax.dynamic_slice(logperm, start, sizes, allow_negative_indices=False)

    parts = [members_of(z)] + [None] * (NZ - 1)
    for d in (4, 1, 7, 2, 6, 3, 5):
        parts[d] = shift_from(members_of(z - d), "z", NZ, d)
    sources = to_mem(strips_kernel, strips, (DEPTH, ROWS_OF, NW), "strips")

    cells, prec, values = lax.sort((obs_cells, obs_prec, obs_values), num_keys=1)
    block = lax.shift_right_logical(cells, BLOCK_BITS)
    counts = jnp.sum(block[None, :] == jnp.arange(NX)[:, None], axis=1).astype(jnp.int32)
    begin = jnp.sum(jnp.where(jnp.arange(NX) < x, counts, 0))
    count = jnp.sum(jnp.where(jnp.arange(NX) == x, counts, 0))
    most = jnp.max(counts)

    def window(done):
        want = jnp.minimum(begin + done, begin + count)
        first = jnp.minimum(want, NOBS - CHUNK)
        stop = jnp.minimum(want + CHUNK, begin + count)
        where = jnp.stack([z, want - first, jnp.maximum(stop - first, 0), mem]).astype(jnp.int32)

        def cut(array):
            return lax.dynamic_slice(array, (first,), (CHUNK,), allow_negative_indices=False)

        at = cut(cells)
        half = lax.shift_right_logical(at, 7) & (HALVES - 1)
        spots = half * (DEPTH * NY) + (lax.shift_right_logical(at, 8) & (DEPTH * NY - 1))
        place = jnp.arange(CHUNK, dtype=jnp.int32)
        lanes = jnp.where((place >= where[1]) & (place < where[2]), at & 127, -1)
        return where, spots, lanes, cut(prec)[None], cut(values)[None]

    where, spots_0, lanes_0, prec_0, values_0 = window(0)
    edge = shape(SUB, HALO, NY, NW)
    first, last = call(
        edges_kernel,
        [edge, edge],
        [jnp.reshape(z, (1,)).astype(jnp.int32), *parts],
        [SM] + [ANY] * NZ,
        [VM, VM],
        [
            pltpu.VMEM((2 * HALO // LAY, SUB, LAY, NY, NW), F32),
            pltpu.SemaphoreType.DMA((2 * HALO // LAY,)),
        ],
        BIG,
        4 * BIG,
        "ends",
    )
    up = [(i, i + 1) for i in range(NX - 1)]
    down = [(i + 1, i) for i in range(NX - 1)]
    h_left, h_right = lax.ppermute(last, "x", up), lax.ppermute(first, "x", down)
    s_left = lax.ppermute(sources[:, DEPTH - HALO :], "x", up)
    s_right = lax.ppermute(sources[:, :HALO], "x", down)

    sent, pred = sweep(
        where, spots_0, lanes_0, h_left, h_right, sources, s_left, s_right, *parts
    )

    def group_preds(parts):
        dims = (CHUNK // 128, MEM, 128)
        return call(preds_kernel, shape(*dims), [parts], [VM], VM, [], 2**20, 2**20, "preds")

    def gram_of(first, parts, prec_cut, value_cut):
        return call(
            gram_kernel,
            shape(M + 8, M),
            [jnp.reshape(first, (1,)).astype(jnp.int32), *parts, prec_cut, value_cut],
            [SM] + [VM] * (NMEM + 2),
            VM,
            [pltpu.VMEM((NMEM, CHUNK // 128, MEM, 128), F32)],
            2 * M * M * CHUNK,
            4 * M * CHUNK,
            "gram",
        )

    def more(carry):
        done, total = carry
        where_n, spots_n, lanes_n, prec_n, values_n = window(done)
        pred_n = call(
            more_kernel,
            PRED,
            [where_n, spots_n, lanes_n, sent],
            [SM] * 3 + [VM],
            VM,
            [PRESSED, FOUND],
            BIG,
            8 * BIG,
            "more",
        )
        group = group_preds(lax.all_gather(pred_n[0], "z"))
        groups = lax.all_gather(group, ("y", "core"))
        split = [groups[g] for g in range(NMEM)]
        return done + CHUNK, total + gram_of(jnp.int32(0), split, prec_n, values_n)

    gathered = exchange(pred, "z")
    groups = round_mem(group_preds(gathered))
    total = gram_of(mem, groups, prec_0, values_0)
    pressure = exchange(sent.reshape(MEM, LAY, NY, NW), "z")
    _, total = lax.while_loop(lambda c: c[0] < most, more, (jnp.int32(CHUNK), total))
    others = [shift_from(total, "x", NX, d) for d in range(1, NX)]

    analysis = analyse(where, [total, *others], states)
    return pressure, analysis


def solution(mesh):
    fine = Mesh(mesh.devices.reshape(NX, NZ, NMEM // 2, 2), ("x", "z", "y", "core"))
    cell, mem = ("x", "z"), ("y", "core")
    return jax.shard_map(
        body,
        mesh=fine,
        in_specs=(P(mem, cell, None, None), P(cell, None, None), P(), P(), P()),
        out_specs=(P(mem, cell, None, None), P(mem, cell, None, None)),
        check_vma=False,
    )
```

```python
import jax
import jax.numpy as jnp
from jax import lax
from jax.experimental import pallas as pl
from jax.experimental.pallas import tpu as pltpu
from jax.sharding import Mesh
from jax.sharding import PartitionSpec as P

M = 128
NOBS = 4096
NS_STEPS = 10
CPRESS = 0.05
HIGH = lax.Precision.HIGHEST
F32 = jnp.float32

NX, NZ, NMEM = 4, 8, 8
LAY = 2
MEM = M // NMEM
SUB = MEM // NZ
DEPTH = NZ * LAY
HALO = 4
FULL = DEPTH + 2 * HALO
GROUP = 4
ROOM = FULL + 6
NY, NW = 64, 256
HALVES = NW // 128
ROWS_OF = NY // NMEM
CHUNK = 1280
BLOCK_BITS = 18

VM = pl.BlockSpec(memory_space=pltpu.VMEM)
SM = pl.BlockSpec(memory_space=pltpu.SMEM)
ANY = pl.BlockSpec(memory_space=pl.ANY)
HBM = pl.BlockSpec(memory_space=pltpu.HBM)


def shape(*dims):
    return jax.ShapeDtypeStruct(dims, F32)


LIMITS = {"ends": 8, "sweeps": 63, "analysis": 32, "more": 16}


def call(kernel, outs, ins, specs, out_specs, scratch, flops, moved, name):
    return pl.pallas_call(
        kernel,
        out_shape=outs,
        in_specs=specs,
        out_specs=out_specs,
        scratch_shapes=scratch,
        cost_estimate=pl.CostEstimate(flops=flops, bytes_accessed=moved, transcendentals=0),
        compiler_params=pltpu.CompilerParams(vmem_limit_bytes=LIMITS.get(name, 8) * 2**20),
    )(*ins)


def root(value):
    return jnp.exp(0.5 * value)


def edges_kernel(where, *refs):
    parts, (first_ref, last_ref, buffer, sems) = refs[:NZ], refs[NZ:]
    ends = HALO // LAY

    def for_ends(act):
        for d in range(NZ):
            slab = (where[0] + d) & (NZ - 1)
            spot = jnp.where(slab < ends, slab, slab - (NZ - 2 * ends))

            @pl.when((slab < ends) | (slab >= NZ - ends))
            def _():
                act(pltpu.make_async_copy(parts[d], buffer.at[spot], sems.at[spot]))

    for_ends(lambda copy: copy.start())
    for_ends(lambda copy: copy.wait())
    for spot in range(ends):
        for m in range(SUB):
            layers = pl.ds(spot * LAY, LAY)
            first_ref[m, layers] = root(buffer[spot, m])
            last_ref[m, layers] = root(buffer[ends + spot, m])


TILES = [(i, half) for i in range(NY // 8) for half in range(NW // 128)]


def tile(i, half):
    return pl.ds(8 * i, 8), pl.ds(128 * half, 128)


def lane_sums(q, j, band, sums):
    value = q[pl.ds(j, GROUP)].reshape(GROUP * NY, NW)
    high = value.astype(jnp.bfloat16)
    low = (value - high.astype(F32)).astype(jnp.bfloat16)
    both = jnp.dot(jnp.concatenate([high, low], axis=0), band[...], preferred_element_type=F32)
    both = both[: GROUP * NY] + both[GROUP * NY :]
    sums[pl.ds(j, GROUP)] = both.reshape(GROUP, NY, NW)


def near_sums(q, sums, j):
    row = lax.broadcasted_iota(jnp.int32, (8, 128), 0)
    middle = {t: q[(j, *tile(*t))] for t in TILES}
    below = {t: pltpu.roll(middle[t], 1, 0) for t in TILES}
    above = {t: pltpu.roll(middle[t], 7, 0) for t in TILES}
    total = {}
    for i, half in TILES:
        t = (i, half)
        side = jnp.where(row == 0, below.get((i - 1, half), 0.0), below[t])
        side = side + jnp.where(row == 7, above.get((i + 1, half), 0.0), above[t])
        side = side + sums[(j, *tile(*t))]
        total[t] = side + (q[(j - 1, *tile(*t))] + q[(j + 1, *tile(*t))])
    return middle, total


def over_layers(q, band, sums, first, groups, step):
    lane_sums(q, first, band, sums)

    @pl.loop(0, groups)
    def _(c):
        j = first + c * GROUP
        lane_sums(q, j + GROUP, band, sums)
        for k in range(GROUP):
            step(j + k)


def gather_all(where, spots, lanes, press, found, copies):
    out = copies.at[0]
    out[...] = jnp.zeros_like(out)
    low, high = where[1] // 128, (where[2] + 127) // 128
    lane = lax.broadcasted_iota(jnp.int32, (1, 128), 1)
    flat = [press.at[m].reshape(HALVES * DEPTH * NY, 128) for m in range(SUB)]

    @pl.loop(low, high)
    def _(k):
        def one(o, carry):
            at = k * 128 + o
            spot, wanted = spots[at], lanes[at]
            for m in range(SUB):
                row = flat[m][pl.ds(spot, 1), :]
                found[m, pl.ds(o, 1), :] = jnp.where(lane == wanted, row, 0.0)
            return carry

        lax.fori_loop(0, 128, one, 0, unroll=16)
        for m in range(SUB):
            out[k, m : m + 1, :] = jnp.sum(found[m].T, axis=0, keepdims=True)

    for copy in range(1, NZ):
        copies[copy] = out[...]


def sweeps_kernel(where, spots, lanes, hl_ref, hr_ref, sources, *refs):
    parts, refs = refs[:NZ], refs[NZ:]
    out, pred_ref, h_all, raw, s_ref, qs, qw, qb, qc, rest, weight, sums, band, *refs = refs
    press, found, sems, in_sems, h_sems, s_sem = refs

    halos = []
    for n, source in enumerate((hl_ref, hr_ref)):
        there = h_all.at[:, pl.ds(1 + n * (HALO + DEPTH), HALO)]
        halos.append(pltpu.make_async_copy(source, there, h_sems.at[n]))
    arrivals = [pltpu.make_async_copy(parts[d], raw.at[d], in_sems.at[d]) for d in range(NZ)]

    strips = [pltpu.make_async_copy(sources, s_ref.at[:, pl.ds(0, FULL)], s_sem)]
    for copy in [*arrivals, *halos, *strips]:
        copy.start()

    def results(m):
        copies = []
        for slab in range(NZ):
            for half in range(HALVES):
                done = press.at[m, half, pl.ds(slab * LAY, LAY)]
                place = out.at[slab, m, :, :, pl.ds(128 * half, 128)]
                copies.append(pltpu.make_async_copy(done, place, sems.at[m, half, slab]))
        return copies

    row = lax.broadcasted_iota(jnp.int32, (NW, NW), 0)
    column = lax.broadcasted_iota(jnp.int32, (NW, NW), 1)
    band[...] = jnp.where(jnp.abs(row - column) == 1, 1.0, 0.0).astype(jnp.bfloat16)
    s_ref[:, FULL : FULL + 2] = jnp.zeros((NMEM, 2, ROWS_OF, NW), F32)
    for m in range(SUB):
        h_all[m, 0] = jnp.zeros((NY, NW), F32)
        h_all[m, FULL + 1 : ROOM] = jnp.zeros((ROOM - FULL - 1, NY, NW), F32)
    for copy in [*arrivals, *halos, *strips]:
        copy.wait()

    @pl.loop(0, SUB)
    def _(m):
        h = h_all.at[m]

        @pl.loop(0, NZ)
        def _(d):
            slab = (where[0] + d) & (NZ - 1)
            for a in range(LAY):
                h[1 + HALO + slab * LAY + a] = root(raw[d, m, a])

        def prepare(j):
            roots, near = near_sums(h, sums, j)
            for i, half in TILES:
                t, spot = (i, half), (j, *tile(i, half))
                inverse = 1.0 / (CPRESS + roots[t] * near[t])
                start = s_ref[i, j - 1, :, pl.ds(128 * half, 128)] * inverse
                slope = roots[t] * inverse
                rest[spot] = start
                weight[spot] = slope
                qs[spot] = roots[t] * start
                qw[spot] = roots[t] * slope

        def sweep_to(new, old):
            def step(j):
                _, near = near_sums(old, sums, j)
                for t in TILES:
                    spot = (j, *tile(*t))
                    new[spot] = qs[spot] + qw[spot] * near[t]

            return step

        def last(j):
            _, near = near_sums(qc, sums, j)
            for i, half in TILES:
                spot = (j, *tile(i, half))
                value = rest[spot] + weight[spot] * near[i, half]
                press[m, half, j - HALO - 1, pl.ds(8 * i, 8), :] = value

        over_layers(h, band, sums, 2, 6, prepare)
        over_layers(qs, band, sums, 3, 5, sweep_to(qb, qs))
        over_layers(qb, band, sums, 4, 5, sweep_to(qc, qb))
        over_layers(qc, band, sums, 5, 4, last)

        for copy in results(m):
            copy.start()

    gather_all(where, spots, lanes, press, found, pred_ref)

    @pl.loop(0, SUB)
    def _(m):
        for copy in results(m):
            copy.wait()


def more_kernel(where, spots, lanes, parts, pred_ref, press, found):
    for slab in range(NZ):
        for m in range(SUB):
            for half in range(HALVES):
                lanes_of = pl.ds(128 * half, 128)
                press[m, half, slab * LAY : slab * LAY + LAY] = parts[slab, m, :, :, lanes_of]
    gather_all(where, spots, lanes, press, found, pred_ref)


def gram_kernel(mem, *refs):
    parts, (prec_ref, value_ref, out_ref, preds) = refs[:NMEM], refs[NMEM:]
    for e in range(NMEM):
        preds[group_at(mem[0], e)] = parts[e][...]
    pred = jnp.concatenate([preds[:, k].reshape(M, 128) for k in range(CHUNK // 128)], axis=1)
    prec = prec_ref[...]
    mean = jnp.sum(pred, axis=0, keepdims=True) * (1.0 / M)
    anomaly = pred - mean
    contract = (((1,), (1,)), ((), ()))
    out_ref[0:M] = lax.dot_general(
        anomaly * prec, anomaly, contract, precision=HIGH, preferred_element_type=F32
    )
    misfit = jnp.broadcast_to(prec * (value_ref[...] - mean), (8, CHUNK))
    out_ref[M : M + 8] = lax.dot_general(
        misfit, anomaly, contract, precision=HIGH, preferred_element_type=F32
    )


def dot(a, b):
    return jnp.dot(a, b, precision=HIGH, preferred_element_type=F32)


PIECES = 8
ROWS = LAY * NY // PIECES


BLOCKS = [(0, 0), (1, 0), (3, 0), (2, 0), (2, MEM // 2)]


def analysis_kernel(where, g0, g1, g2, g3, *refs):
    states, (out, buffer, done, turned, sems, out_sems) = refs[: 2 * len(BLOCKS)], refs[2 * len(BLOCKS) :]

    def place(k, half):
        layer, first = k // (NY // ROWS), pl.multiple_of(k % (NY // ROWS) * ROWS, ROWS)
        return (slice(None), layer, pl.ds(first, ROWS), pl.ds(half * 128, 128))

    def pieces(k, half):
        y, core = where[3] // 2, where[3] & 1
        copies = []
        for n, source in enumerate(states):
            step, first = BLOCKS[n % len(BLOCKS)]
            group = ((y + step) & 3) * 2 + (core if n < len(BLOCKS) else 1 - core)
            rows = pl.ds(group * MEM + first, source.shape[0])
            there = buffer.at[k, half, rows]
            copies.append(pltpu.make_async_copy(source.at[place(k, half)], there, sems.at[k, half, n]))
        return copies

    def result(k, half):
        return pltpu.make_async_copy(
            done.at[k, half], out.at[place(k, half)], out_sems.at[k, half]
        )

    @pl.loop(0, PIECES)
    def _(k):
        for half in range(HALVES):
            for copy in pieces(k, half):
                copy.start()

    sums = (g0[...] + g1[...]) + (g2[...] + g3[...])
    row = lax.broadcasted_iota(jnp.int32, (M, M), 0)
    column = lax.broadcasted_iota(jnp.int32, (M, M), 1)
    identity = jnp.where(row == column, 1.0, 0.0).astype(F32)
    scaled = identity + sums[0:M] / (M - 1)
    bound = jnp.max(jnp.sum(jnp.abs(scaled), axis=1, keepdims=True), axis=0, keepdims=True)
    root = scaled / bound
    inv_root = 1.5 * identity - 0.5 * root
    root = dot(root, inv_root)
    for step in range(1, NS_STEPS):
        factor = 1.5 * identity - 0.5 * dot(inv_root, root)
        if step < NS_STEPS - 1:
            root = dot(root, factor)
        inv_root = dot(factor, inv_root)
    contract = (((1,), (1,)), ((), ()))
    shift = sums[M : M + 8]
    for _ in range(2):
        shift = lax.dot_general(shift, inv_root, contract, precision=HIGH, preferred_element_type=F32)
    shift = shift[0:1] / bound / (M - 1)
    turned[...] = inv_root.T / jnp.sqrt(bound) + shift
    mine = turned[pl.ds(pl.multiple_of(where[3] * MEM, MEM), MEM), :]
    mine = mine + (1.0 - jnp.sum(mine, axis=1, keepdims=True)) * (1.0 / M)
    high = mine.astype(jnp.bfloat16)
    low = (mine - high.astype(F32)).astype(jnp.bfloat16)
    left = jnp.concatenate(
        [
            jnp.concatenate([high, high], axis=1),
            jnp.concatenate([low, jnp.zeros_like(low)], axis=1),
        ],
        axis=0,
    )

    @pl.loop(0, PIECES)
    def _(k):
        for half in range(HALVES):
            for copy in pieces(k, half):
                copy.wait()
        given = [buffer.at[k, half].reshape(M * ROWS, 128) for half in range(HALVES)]
        taken = [done.at[k, half].reshape(MEM * ROWS, 128) for half in range(HALVES)]
        for r in range(ROWS):
            state = jnp.concatenate([g[pl.ds(r, M, stride=ROWS), :] for g in given], axis=1)
            upper = state.astype(jnp.bfloat16)
            lower = (state - upper.astype(F32)).astype(jnp.bfloat16)
            both = jnp.dot(
                left, jnp.concatenate([upper, lower], axis=0), preferred_element_type=F32
            )
            both = both[:MEM] + both[MEM:]
            for half in range(HALVES):
                taken[half][pl.ds(r, MEM, stride=ROWS), :] = both[:, half * 128 : half * 128 + 128]
        for half in range(HALVES):
            result(k, half).start()

    for k in range(PIECES):
        for half in range(HALVES):
            result(k, half).wait()


BIG = SUB * DEPTH * NY * NW
PARTS = shape(NZ, SUB, LAY, NY, NW)
PRED = shape(NZ, CHUNK // 128, SUB, 128)
PRESSED = pltpu.VMEM((SUB, HALVES, DEPTH, NY, 128), F32)
FOUND = pltpu.VMEM((SUB, 128, 128), F32)


def sweep(*ins):
    return call(
        sweeps_kernel,
        [PARTS, PRED],
        ins,
        [SM] * 3 + [ANY] * (3 + NZ),
        [HBM, VM],
        [pltpu.VMEM((SUB, ROOM, NY, NW), F32), pltpu.VMEM((NZ, SUB, LAY, NY, NW), F32)]
        + [pltpu.VMEM((NMEM, FULL + 2, ROWS_OF, NW), F32)]
        + [pltpu.VMEM((ROOM, NY, NW), F32)] * 7
        + [pltpu.VMEM((NW, NW), jnp.bfloat16), PRESSED, FOUND]
        + [pltpu.SemaphoreType.DMA((SUB, HALVES, NZ))]
        + [pltpu.SemaphoreType.DMA((NZ,)), pltpu.SemaphoreType.DMA((2,)), pltpu.SemaphoreType.DMA],
        64 * BIG,
        16 * BIG,
        "sweeps",
    )


def analyse(where, sums, states):
    return call(
        analysis_kernel,
        shape(MEM, LAY, NY, NW),
        [where, *sums, *states],
        [SM] + [VM] * NX + [HBM] * (2 * len(BLOCKS)),
        ANY,
        [
            pltpu.VMEM((PIECES, HALVES, M, ROWS, 128), F32),
            pltpu.VMEM((PIECES, HALVES, MEM, ROWS, 128), F32),
            pltpu.VMEM((M, M), F32),
            pltpu.SemaphoreType.DMA((PIECES, HALVES, 2 * len(BLOCKS))),
            pltpu.SemaphoreType.DMA((PIECES, HALVES)),
        ],
        2 * M * MEM * LAY * NY * NW,
        4 * M * LAY * NY * NW,
        "analysis",
    )


def shift_from(array, axis, size, by):
    return lax.ppermute(array, axis, [((i + by) % size, i) for i in range(size)])


def exchange(copies, axis):
    return lax.all_to_all(copies, axis, 0, 0, tiled=True)


def strip_kernel(mem, source, out, sems):
    copies = []
    for slab in range(NZ):
        rows = source.at[:, pl.ds(pl.multiple_of(mem[0] * ROWS_OF, ROWS_OF), ROWS_OF)]
        copies.append(pltpu.make_async_copy(rows, out.at[slab], sems.at[slab]))
    for copy in copies:
        copy.start()
    for copy in copies:
        copy.wait()


def strips_kernel(left, strips, right, out):
    parts = [left[n] for n in range(HALO // LAY)]
    parts += [strips[n] for n in range(NZ)]
    parts += [right[n] for n in range(HALO // LAY)]
    for copy in range(NMEM):
        for n, part in enumerate(parts):
            out[copy, LAY * n : LAY * n + LAY] = part


def preds_kernel(parts, out):
    for g in range(NZ):
        for m in range(SUB):
            for k in range(CHUNK // 128):
                row = g * SUB + m
                out[k, row : row + 1, :] = parts[g, k, m : m + 1, :]


def group_at(mem, e):
    return (((mem // 2 + e // 2) & (NMEM // 2 - 1)) * 2) + ((mem & 1) ^ (e & 1))


def round_mem(array):
    parts = [array]
    for e in range(1, NMEM):
        pairs = [(group_at(i, e), i) for i in range(NMEM)]
        parts.append(lax.ppermute(array, ("y", "core"), pairs))
    return parts


def body(logperm, source, obs_cells, obs_values, obs_prec):
    x, z, mem = lax.axis_index("x"), lax.axis_index("z"), lax.axis_index(("y", "core"))

    def swapped(array):
        return lax.ppermute(array, "core", [(0, 1), (1, 0)])

    half = MEM // 2
    after, before = shift_from(logperm, "y", 4, 1), shift_from(logperm, "y", 4, 3)
    far_a, far_b = shift_from(after[:half], "y", 4, 1), shift_from(before[half:], "y", 4, 3)
    others = [swapped(array) for array in (logperm, after, before)]
    others += [swapped(array) for array in (far_a, far_b)]
    states = [logperm, after, before, far_a, far_b, *others]

    strip = call(
        strip_kernel,
        pltpu.HBM((NZ, LAY, ROWS_OF, NW), F32),
        [jnp.reshape(mem, (1,)).astype(jnp.int32), source],
        [SM, VM],
        HBM,
        [pltpu.SemaphoreType.DMA((NZ,))],
        2**20,
        2**20,
        "strip",
    )
    strips = exchange(strip, "z")
    up = [(i, i + 1) for i in range(NX - 1)]
    down = [(i + 1, i) for i in range(NX - 1)]
    s_left = lax.ppermute(strips[NZ - HALO // LAY :], "x", up)
    s_right = lax.ppermute(strips[: HALO // LAY], "x", down)

    def members_of(group):
        start = ((group & (NZ - 1)) * SUB, 0, 0, 0)
        sizes = (SUB, LAY, NY, NW)
        return lax.dynamic_slice(logperm, start, sizes, allow_negative_indices=False)

    parts = [members_of(z)] + [None] * (NZ - 1)
    for d in (4, 1, 7, 2, 6, 3, 5):
        parts[d] = shift_from(members_of(z - d), "z", NZ, d)
    copies = call(
        strips_kernel,
        shape(NMEM, FULL, ROWS_OF, NW),
        [s_left, strips, s_right],
        [VM] * 3,
        VM,
        [],
        2**20,
        2**20,
        "strips",
    )
    sources = exchange(copies, ("y", "core"))

    cells, prec, values = lax.sort((obs_cells, obs_prec, obs_values), num_keys=1)
    block = lax.shift_right_logical(cells, BLOCK_BITS)
    counts = jnp.sum(block[None, :] == jnp.arange(NX)[:, None], axis=1).astype(jnp.int32)
    begin = jnp.sum(jnp.where(jnp.arange(NX) < x, counts, 0))
    count = jnp.sum(jnp.where(jnp.arange(NX) == x, counts, 0))
    most = jnp.max(counts)

    def window(done):
        want = jnp.minimum(begin + done, begin + count)
        first = jnp.minimum(want, NOBS - CHUNK)
        stop = jnp.minimum(want + CHUNK, begin + count)
        where = jnp.stack([z, want - first, jnp.maximum(stop - first, 0), mem]).astype(jnp.int32)

        def cut(array):
            return lax.dynamic_slice(array, (first,), (CHUNK,), allow_negative_indices=False)

        at = cut(cells)
        half = lax.shift_right_logical(at, 7) & (HALVES - 1)
        spots = half * (DEPTH * NY) + (lax.shift_right_logical(at, 8) & (DEPTH * NY - 1))
        place = jnp.arange(CHUNK, dtype=jnp.int32)
        lanes = jnp.where((place >= where[1]) & (place < where[2]), at & 127, -1)
        return where, spots, lanes, cut(prec)[None], cut(values)[None]

    where, spots_0, lanes_0, prec_0, values_0 = window(0)
    edge = shape(SUB, HALO, NY, NW)
    first, last = call(
        edges_kernel,
        [edge, edge],
        [jnp.reshape(z, (1,)).astype(jnp.int32), *parts],
        [SM] + [ANY] * NZ,
        [VM, VM],
        [
            pltpu.VMEM((2 * HALO // LAY, SUB, LAY, NY, NW), F32),
            pltpu.SemaphoreType.DMA((2 * HALO // LAY,)),
        ],
        BIG,
        4 * BIG,
        "ends",
    )
    h_left, h_right = lax.ppermute(last, "x", up), lax.ppermute(first, "x", down)
    sent, pred = sweep(
        where, spots_0, lanes_0, h_left, h_right, sources, *parts
    )

    def group_preds(parts):
        dims = (CHUNK // 128, MEM, 128)
        return call(preds_kernel, shape(*dims), [parts], [VM], VM, [], 2**20, 2**20, "preds")

    def gram_of(first, parts, prec_cut, value_cut):
        return call(
            gram_kernel,
            shape(M + 8, M),
            [jnp.reshape(first, (1,)).astype(jnp.int32), *parts, prec_cut, value_cut],
            [SM] + [VM] * (NMEM + 2),
            VM,
            [pltpu.VMEM((NMEM, CHUNK // 128, MEM, 128), F32)],
            2 * M * M * CHUNK,
            4 * M * CHUNK,
            "gram",
        )

    def more(carry):
        done, total = carry
        where_n, spots_n, lanes_n, prec_n, values_n = window(done)
        pred_n = call(
            more_kernel,
            PRED,
            [where_n, spots_n, lanes_n, sent],
            [SM] * 3 + [VM],
            VM,
            [PRESSED, FOUND],
            BIG,
            8 * BIG,
            "more",
        )
        group = group_preds(lax.all_gather(pred_n[0], "z"))
        groups = lax.all_gather(group, ("y", "core"))
        split = [groups[g] for g in range(NMEM)]
        return done + CHUNK, total + gram_of(jnp.int32(0), split, prec_n, values_n)

    gathered = exchange(pred, "z")
    groups = round_mem(group_preds(gathered))
    total = gram_of(mem, groups, prec_0, values_0)
    pressure = exchange(sent.reshape(MEM, LAY, NY, NW), "z")
    _, total = lax.while_loop(lambda c: c[0] < most, more, (jnp.int32(CHUNK), total))
    others = [shift_from(total, "x", NX, d) for d in range(1, NX)]

    analysis = analyse(where, [total, *others], states)
    return pressure, analysis


def solution(mesh):
    fine = Mesh(mesh.devices.reshape(NX, NZ, NMEM // 2, 2), ("x", "z", "y", "core"))
    cell, mem = ("x", "z"), ("y", "core")
    return jax.shard_map(
        body,
        mesh=fine,
        in_specs=(P(mem, cell, None, None), P(cell, None, None), P(), P(), P()),
        out_specs=(P(mem, cell, None, None), P(mem, cell, None, None)),
        check_vma=False,
    )
```
